32 devices in a mesh: chain: 16 (over z, x, core), dp: 2 (over y).
Axes of the slice: x: 2, y: 2, z: 4, core: 2. Of those that a mesh axis runs over, the one named last changes fastest.
Arguments:
- segments: bfloat16 [2, 16, 128, 1024], P('dp', 'chain'), may hold values from -6 to 6
- lengths: int32 [2, 16], P('dp', 'chain'), may hold values from 64 to 128, as said below
- query_weight: bfloat16 [1024, 1024], replicated, may hold values from -0.1875 to 0.1875
- key_weight: bfloat16 [1024, 256], replicated, may hold values from -0.1875 to 0.1875
- value_weight: bfloat16 [1024, 256], replicated, may hold values from -0.1875 to 0.1875
- out_weight: bfloat16 [1024, 1024], replicated, may hold values from -0.1875 to 0.1875
- norm_gain: float32 [1024], replicated, may hold values from 0.5 to 1.5
- gate_vector: float32 [1024], replicated, may hold values from -0.6 to 0.6
- gate_bias: float32 [128], replicated, may hold values from -2 to 5
- memory_init: bfloat16 [128, 1024], replicated, may hold values from -6 to 6
- cotangent: bfloat16 [2, 16, 128, 1024], P('dp', 'chain'), may hold values from -6 to 6
Outputs:
- layer_output: bfloat16 [2, 16, 128, 1024], P('dp', 'chain')
- grad_query: float32 [1024, 1024], P(('chain', 'dp'))
- grad_key: float32 [1024, 256], P(('chain', 'dp'))
- grad_value: float32 [1024, 256], P(('chain', 'dp'))
- grad_out: float32 [1024, 1024], P(('chain', 'dp'))
- grad_gain: float32 [1024], P(('chain', 'dp'))
- grad_gate: float32 [1024], P(('chain', 'dp'))
- grad_memory: float32 [128, 1024], P(None, ('chain', 'dp'))
The draws below stay inside these ranges and needn't reach their ends.
Inputs may be any that keep to these rules, and one draw needn't show every extreme that they name: `lengths`: in every document one segment is full.
All inputs are finite; a program needn't handle non-finite values.
Results may differ from the reference program's by a relative error of at most 0.02.
Values sent between devices are 32-bit elements; how exact they have to be, the bound alone decides.
No kernel may reach another device: no remote copies, remote signals or barrier semaphores. Data moves between devices by JAX's collectives and lax.ppermute only.
A program may use at most 128 MiB of HBM per device.

```python
import jax
import jax.numpy as jnp
from jax import lax

D = 1024
HEAD = 64
QHEADS = 16
KVHEADS = 4
MEM = 128
SEG = 128
DOCS = 2
SEGS = 16


def draw_lengths(key, part):
    base = jax.random.randint(key, (DOCS, SEGS), SEG // 2, SEG + 1)
    chosen = jax.random.randint(jax.random.fold_in(key, 7), (DOCS, 1), 0, SEGS)
    return jnp.where(jnp.arange(SEGS)[None, :] == chosen, SEG, base).astype(jnp.int32)


def spiked(entries, key, source, target, shards_of, factor):
    def block_of(position):
        return (jnp.arange(entries.shape[position]) // (entries.shape[position] // shards_of)).reshape((-1,) + (1,) * (entries.ndim - 1 - position))

    one_side = jax.random.permutation(key, shards_of)[block_of(target)]
    second = (block_of(target) + shards_of // 2) % shards_of
    return jnp.where((block_of(source) == one_side) | (block_of(source) == second), factor * entries, entries)


def steps_of(rng, dims, split, least, largest):
    gain = 1.0
    for axis_at, blocks in split:
        heights = jax.random.uniform(jax.random.fold_in(jax.random.fold_in(rng, 6), axis_at), (blocks,), jnp.float32, least / len(split), largest / len(split))
        gain = gain * jnp.repeat(jnp.exp(heights), dims[axis_at] // blocks).reshape((-1,) + (1,) * (len(dims) - 1 - axis_at))
    return gain


def noise(key, shape, scale, most, split=(), kind=jnp.bfloat16):
    gain = steps_of(key, shape, split, -0.22, 0.18) if split else 1.0
    array = jax.random.normal(key, shape, jnp.float32) * scale * gain
    return jnp.minimum(jnp.maximum(array, -most), most).astype(kind)


def noise_with(key, shape, scale, reach, split, heavy, held_as=jnp.bfloat16):
    drawn = scale * jax.random.normal(key, shape, jnp.float32)
    if split:
        drawn = drawn * steps_of(key, shape, split, -0.22, 0.18)
    return jnp.clip(spiked(drawn, jax.random.fold_in(key, 3), *heavy), -reach, reach).astype(held_as)


def setup_inputs(seed: int = 0) -> dict:
    streams_of = jax.random.split(jax.random.key(seed), 12)
    return {
        "segments": noise_with(streams_of[0], (DOCS, SEGS, SEG, D), 1.0, 6.0, ((0, 2), (1, 16)), (1, 3, 16, 2.0)),
        "lengths": draw_lengths(jax.random.fold_in(streams_of[11], 71), 0),
        "query_weight": noise(streams_of[2], (D, QHEADS * HEAD), D ** -0.5, 0.1875),
        "key_weight": noise(streams_of[3], (D, KVHEADS * HEAD), D ** -0.5, 0.1875),
        "value_weight": noise(streams_of[4], (D, KVHEADS * HEAD), D ** -0.5, 0.1875),
        "out_weight": noise(streams_of[5], (QHEADS * HEAD, D), (QHEADS * HEAD) ** -0.5, 0.1875),
        "norm_gain": jnp.clip(1.0 + 0.1 * jax.random.normal(streams_of[6], (D,), jnp.float32), 0.5, 1.5),
        "gate_vector": noise(streams_of[7], (D,), 0.1, 0.6, (), jnp.float32),
        "gate_bias": jnp.clip(jax.random.uniform(streams_of[8], (MEM,), jnp.float32, -2.0, 5.0), -2.0, 5.0),
        "memory_init": noise(streams_of[9], (MEM, D), 1.0, 6.0),
        "cotangent": noise_with(streams_of[10], (DOCS, SEGS, SEG, D), 1.0, 6.0, ((0, 2), (1, 16)), (1, 3, 16, 2.0)),
    }


epsilon = 1e-05
score_scale = 0.125

def normalize(activations, norm_gain):
    inverse = lax.rsqrt(lax.optimization_barrier(jnp.mean(activations * activations, axis=-1, keepdims=True)) + epsilon)
    return (activations * inverse * norm_gain).astype(jnp.bfloat16)

def prepare(query_weight, key_weight, value_weight, norm_gain, segment):
    normed_rows = normalize(segment.astype(jnp.float32), norm_gain)
    queries = (jnp.dot(normed_rows, query_weight, preferred_element_type=jnp.float32) * score_scale).astype(jnp.bfloat16)
    key_rows = jnp.dot(normed_rows, key_weight, preferred_element_type=jnp.float32).astype(jnp.bfloat16)
    value_rows = jnp.dot(normed_rows, value_weight, preferred_element_type=jnp.float32).astype(jnp.bfloat16)
    return (queries, key_rows, value_rows)

def attend(queries, key_rows, value_rows, allowed):
    count = queries.shape[0]
    width = key_rows.shape[0]
    groups = key_rows.shape[1] // HEAD
    shared = queries.shape[1] // key_rows.shape[1]
    grouped = queries.reshape(count, groups, shared, HEAD)
    keyed = key_rows.reshape(width, groups, HEAD)
    valued = value_rows.reshape(width, groups, HEAD)
    scores = jnp.einsum('rgsh,kgh->gsrk', grouped, keyed, preferred_element_type=jnp.float32)
    scores = jnp.where(allowed, scores, -1e+30)
    weights = jax.nn.softmax(scores, axis=-1).astype(jnp.bfloat16)
    context = jnp.einsum('gsrk,kgh->rgsh', weights, valued, preferred_element_type=jnp.float32)
    return context.reshape(count, groups * shared * HEAD).astype(jnp.bfloat16)

def read_part(queries, seg_keys, seg_values, key_weight, value_weight, out_weight, norm_gain, memory_in, segment, seg_length):
    memory_rows = normalize(memory_in, norm_gain)
    memory_keys = jnp.dot(memory_rows, key_weight, preferred_element_type=jnp.float32).astype(jnp.bfloat16)
    memory_values = jnp.dot(memory_rows, value_weight, preferred_element_type=jnp.float32).astype(jnp.bfloat16)
    key_rows = jnp.concatenate([memory_keys, seg_keys], axis=0)
    value_rows = jnp.concatenate([memory_values, seg_values], axis=0)
    count = segment.shape[0]
    places = jnp.arange(count)
    causal = (places[None, :] <= places[:, None]) & (places[None, :] < seg_length)
    allowed = jnp.concatenate([jnp.ones((count, memory_in.shape[0]), dtype=bool), causal], axis=1)
    context = attend(queries, key_rows, value_rows, allowed)
    return segment.astype(jnp.float32) + jnp.dot(context, out_weight, preferred_element_type=jnp.float32)

def write_part(seg_keys, seg_values, query_weight, out_weight, norm_gain, gate_vector, memory_start, gate_bias, seg_length):
    start_rows = normalize(memory_start, norm_gain)
    slot_queries = (jnp.dot(start_rows, query_weight, preferred_element_type=jnp.float32) * score_scale).astype(jnp.bfloat16)
    places = jnp.arange(seg_keys.shape[0])
    allowed = jnp.broadcast_to(places[None, :] < seg_length, (memory_start.shape[0], seg_keys.shape[0]))
    context = attend(slot_queries, seg_keys, seg_values, allowed)
    written = jnp.dot(context, out_weight, preferred_element_type=jnp.float32)
    retain = jax.nn.sigmoid(gate_bias + jnp.dot(written, gate_vector, precision=lax.Precision.HIGHEST))
    return (retain, written)

def reference(segments, lengths, query_weight, key_weight, value_weight, out_weight, norm_gain, gate_vector, gate_bias, memory_init, cotangent):
    memory_start = memory_init.astype(jnp.float32)

    def document(bundle):
        seg_rows, seg_lengths, seg_cotangents = bundle

        def forward_write(paired):
            segment, seg_length = paired
            queries, seg_keys, seg_values = prepare(query_weight, key_weight, value_weight, norm_gain, segment)
            return write_part(seg_keys, seg_values, query_weight, out_weight, norm_gain, gate_vector, memory_start, gate_bias, seg_length)
        retain_all, written_all = lax.map(forward_write, (seg_rows, seg_lengths))

        def advance(memory, paired):
            retain, written = paired
            return (retain[:, None] * memory + (1.0 - retain)[:, None] * written, memory)
        unused, memory_all = lax.scan(advance, memory_start, (retain_all, written_all))

        def backward_read(bundle_in):
            segment, seg_length, memory_in, seg_cot = bundle_in
            queries, seg_keys, seg_values = prepare(query_weight, key_weight, value_weight, norm_gain, segment)

            def reading(queries_in, keys_in, values_in, key_part, value_part, out_part, gain_part, memory_part):
                return read_part(queries_in, keys_in, values_in, key_part, value_part, out_part, gain_part, memory_part, segment, seg_length)
            result, read_back = jax.vjp(reading, queries, seg_keys, seg_values, key_weight, value_weight, out_weight, norm_gain, memory_in)
            valid_rows = (jnp.arange(segment.shape[0]) < seg_length)[:, None]
            gradients = read_back(seg_cot.astype(jnp.float32) * valid_rows)
            return (result.astype(jnp.bfloat16),) + tuple(gradients)
        read_out = lax.map(backward_read, (seg_rows, seg_lengths, memory_all, seg_cotangents))
        layer_out, d_queries, d_keys_read, d_values_read, key_read, value_read, out_read, gain_read, d_memory = read_out

        def upstream(later_grad, paired):
            retain, local_grad = paired
            return (local_grad + retain[:, None] * later_grad, later_grad)
        anchor_grad, later_all = lax.scan(upstream, jnp.zeros_like(memory_start), (retain_all, d_memory), reverse=True)

        def backward_write(totals, bundle_in):
            segment, seg_length, memory_in, retain, written, later_grad, dq_in, dk_in, dv_in = bundle_in

            def prepared(query_part, key_part, value_part, gain_part):
                return prepare(query_part, key_part, value_part, gain_part, segment)
            (queries, seg_keys, seg_values), prep_back = jax.vjp(prepared, query_weight, key_weight, value_weight, norm_gain)

            def writing(keys_in, values_in, query_part, out_part, gain_part, vector_part, start_part):
                return write_part(keys_in, values_in, query_part, out_part, gain_part, vector_part, start_part, gate_bias, seg_length)
            unused_pair, write_back = jax.vjp(writing, seg_keys, seg_values, query_weight, out_weight, norm_gain, gate_vector, memory_start)
            d_retain = lax.optimization_barrier(jnp.sum(later_grad * (memory_in - written), axis=1))
            d_written = (1.0 - retain)[:, None] * later_grad
            d_keys_write, d_values_write, query_write, out_write, gain_write, gate_grad, start_grad = write_back((d_retain, d_written))
            d_keys = (dk_in.astype(jnp.float32) + d_keys_write.astype(jnp.float32)).astype(jnp.bfloat16)
            d_values = (dv_in.astype(jnp.float32) + d_values_write.astype(jnp.float32)).astype(jnp.bfloat16)
            query_prep, key_prep, value_prep, gain_prep = prep_back((dq_in, d_keys, d_values))
            updates = (query_write.astype(jnp.float32) + query_prep.astype(jnp.float32), key_prep.astype(jnp.float32), value_prep.astype(jnp.float32), out_write.astype(jnp.float32), gain_write + gain_prep, gate_grad, start_grad)
            return (tuple((total + update for total, update in zip(totals, updates))), None)
        zeros_init = (jnp.zeros(query_weight.shape, jnp.float32), jnp.zeros(key_weight.shape, jnp.float32), jnp.zeros(value_weight.shape, jnp.float32), jnp.zeros(out_weight.shape, jnp.float32), jnp.zeros(norm_gain.shape, jnp.float32), jnp.zeros(gate_vector.shape, jnp.float32), jnp.zeros(memory_start.shape, jnp.float32))
        totals, unused_rows = lax.scan(backward_write, zeros_init, (seg_rows, seg_lengths, memory_all, retain_all, written_all, later_all, d_queries, d_keys_read, d_values_read))
        grads = (totals[0], totals[1] + lax.optimization_barrier(jnp.sum(key_read.astype(jnp.float32), axis=0)), totals[2] + lax.optimization_barrier(jnp.sum(value_read.astype(jnp.float32), axis=0)), totals[3] + lax.optimization_barrier(jnp.sum(out_read.astype(jnp.float32), axis=0)), totals[4] + lax.optimization_barrier(jnp.sum(gain_read, axis=0)), totals[5], totals[6] + anchor_grad)
        return (layer_out,) + grads
    results = lax.map(document, (segments, lengths, cotangent))
    sums = tuple((lax.optimization_barrier(jnp.sum(item, axis=0)) for item in results[1:]))
    return (results[0], sums[0], sums[1], sums[2], sums[3], sums[4], sums[5], sums[6])
```

```python
import functools

import jax
import jax.numpy as jnp
from jax import lax
from jax.experimental import pallas as pl
from jax.experimental.pallas import tpu as pltpu
from jax.sharding import PartitionSpec as P

HEAD = 64
LANES = 128
epsilon = 1e-05
score_scale = 0.125
F32 = jnp.float32
BF16 = jnp.bfloat16


def mm(a, b):
    return lax.dot_general(a, b, (((1,), (0,)), ((), ())), preferred_element_type=F32)


def mm_nt(a, b):
    return lax.dot_general(a, b, (((1,), (1,)), ((), ())), preferred_element_type=F32)


def inverse_rms(rows):
    return lax.rsqrt(jnp.mean(rows * rows, axis=-1, keepdims=True) + epsilon)


def low_lanes(shape):
    return lax.broadcasted_iota(jnp.int32, shape, 1) < HEAD


def padded(tile, odd):
    wide = tile.astype(F32)
    mine = low_lanes(wide.shape) != bool(odd)
    here = jnp.where(mine, wide, 0.0)
    there = pltpu.roll(here, HEAD, 1)
    low, high = (there, here) if odd else (here, there)
    return jnp.concatenate([low, high], axis=0).astype(BF16)


def unpadded(total, odd):
    rows = total.shape[0] // 2
    low_mask = low_lanes((rows, LANES))
    low = jnp.where(low_mask, total[:rows], 0.0)
    high = jnp.where(low_mask, 0.0, total[rows:])
    return high + pltpu.roll(low, HEAD, 1) if odd else low + pltpu.roll(high, HEAD, 1)


def softmax_rows(scores, allowed):
    width = scores.shape[0] // 2
    halves = []
    for part in (scores[:width], scores[width:]):
        part = jnp.where(allowed, part, -1e30)
        raised = jnp.exp(part - jnp.max(part, axis=0, keepdims=True))
        halves.append(raised / jnp.sum(raised, axis=0, keepdims=True))
    return jnp.concatenate(halves, axis=0)


def softmax_back(weights, d_weights):
    width = weights.shape[0] // 2
    halves = []
    for at in (0, width):
        w, d = weights[at : at + width], d_weights[at : at + width]
        halves.append(w * (d - jnp.sum(w * d, axis=0, keepdims=True)))
    return jnp.concatenate(halves, axis=0)


def split3(value):
    high = value.astype(BF16)
    rest = value - high.astype(F32)
    mid = rest.astype(BF16)
    return high, mid, (rest - mid.astype(F32)).astype(BF16)


def row_times(row, matrix, transposed):
    pieces = split3(row)
    stacked = jnp.concatenate(list(pieces) + [jnp.zeros_like(pieces[0])] * 13, axis=0)
    return jnp.sum((mm_nt if transposed else mm)(stacked, matrix), axis=0, keepdims=True)


def prepare_kernel(
    length, seg, wq, wk, wv, wo, gain, vector, mem0, xn_o, q_o, kv_o, sn_o, s_o, c_o, u_o
):
    count = seg.shape[0]
    kv_width = wk.shape[1]
    rows = seg[...].astype(F32)
    start = mem0[...].astype(F32)
    g = gain[...]
    xn = (rows * inverse_rms(rows) * g).astype(BF16)
    sn = (start * inverse_rms(start) * g).astype(BF16)
    xn_o[...] = xn
    sn_o[...] = sn
    both = mm(jnp.concatenate([xn, sn], axis=0), wq[...]) * score_scale
    q_o[...] = both[:count].astype(BF16)
    s_o[...] = both[count:].astype(BF16)
    kv_o[:, :kv_width] = mm(xn, wk[...]).astype(BF16)
    kv_o[:, kv_width:] = mm(xn, wv[...]).astype(BF16)
    u_o[...] = row_times(vector[...], wo[...], True)
    slots = mem0.shape[0]
    allowed = lax.broadcasted_iota(jnp.int32, (count, slots), 0) < length[0, 0]
    pairs = s_o.shape[1] // LANES
    groups = kv_width // HEAD
    for group in range(groups):
        at, odd = (group // 2) * LANES, group % 2
        keys = padded(kv_o[:, at : at + LANES], odd)
        values_t = padded(kv_o[:, kv_width + at : kv_width + at + LANES], odd).T
        for pair in range(group * pairs // groups, (group + 1) * pairs // groups):
            lanes = slice(pair * LANES, (pair + 1) * LANES)
            weights = softmax_rows(mm_nt(keys, s_o[:, lanes]), allowed).astype(BF16)
            c_o[:, lanes] = mm(values_t, weights).T.astype(BF16).astype(F32)


def owner_kernel(
    call, bias, mem_own, u, wo, wk, wv, gain, p_o, mem_o, stat_o, mn_o, mkv_o, *, chain
):
    rows = call.shape[0]
    own = rows // chain
    logits = jnp.sum(call[...] * u[...], axis=1, keepdims=True) + bias[...]
    retain = jax.nn.sigmoid(logits)
    stat_o[0] = jnp.broadcast_to(retain, (rows, LANES))
    memory = jnp.zeros((own, call.shape[1]), F32)
    keep = jnp.ones((own, LANES), F32)
    for c in range(chain):
        at = slice(c * own, (c + 1) * own)
        p_o[at, :] = memory
        stat_o[1, at, :] = keep
        ret = stat_o[0, at, :]
        memory = ret[:, :1] * memory + (1.0 - ret[:, :1]) * call[at, :]
        keep = keep * ret
    start = jnp.concatenate([mem_own[...]] * chain, axis=0)
    mem = stat_o[1][:, :1] * start + mm(p_o[...].astype(BF16), wo[...])
    mem_o[...] = mem
    inverse = inverse_rms(mem)
    stat_o[2] = jnp.broadcast_to(inverse, (rows, LANES))
    mn = (mem * inverse * gain[...]).astype(BF16)
    mn_o[...] = mn
    width = wk.shape[1]
    mkv_o[:, :width] = mm(mn, wk[...]).astype(BF16).astype(F32)
    mkv_o[:, width:] = mm(mn, wv[...]).astype(BF16).astype(F32)


def read_kernel(
    length, seg, cot, q, kv, mkv, wo, out_o, cr_o, do_o, dq_o, dkv_o, dmkv_o, dcr_s, w_s
):
    count, width = q.shape
    slots = mkv.shape[0]
    kv_width = kv.shape[1] // 2
    pairs = width // LANES
    groups = kv_width // HEAD
    valid = lax.broadcasted_iota(jnp.int32, (count, 1), 0) < length[0, 0]
    d_out = jnp.where(valid, cot[...].astype(F32), 0.0).astype(BF16)
    do_o[...] = d_out
    dcr_s[...] = mm_nt(d_out, wo[...]).astype(BF16)
    key_at = lax.broadcasted_iota(jnp.int32, (slots + count, count), 0) - slots
    query_at = lax.broadcasted_iota(jnp.int32, (slots + count, count), 1)
    allowed = (key_at < 0) | ((key_at <= query_at) & (key_at < length[0, 0]))
    d_keys = [None] * groups
    d_values = [None] * groups
    for group in range(groups):
        at, odd = (group // 2) * LANES, group % 2
        keys = padded(
            jnp.concatenate(
                [mkv[:, at : at + LANES], kv[:, at : at + LANES].astype(F32)], axis=0
            ),
            odd,
        )
        at_v = kv_width + at
        values = padded(
            jnp.concatenate(
                [mkv[:, at_v : at_v + LANES], kv[:, at_v : at_v + LANES].astype(F32)], axis=0
            ),
            odd,
        )
        keys_t, values_t = keys.T, values.T
        dk = dv = None
        for pair in range(group * pairs // groups, (group + 1) * pairs // groups):
            lanes = slice(pair * LANES, (pair + 1) * LANES)
            q_tile = q[:, lanes]
            weights = softmax_rows(mm_nt(keys, q_tile), allowed)
            rounded = weights.astype(BF16)
            cr_o[:, lanes] = mm(values_t, rounded).T.astype(BF16)
            d_tile = dcr_s[:, lanes]
            d_weights = mm_nt(values, d_tile).astype(BF16).astype(F32)
            d_scores = softmax_back(weights, d_weights).astype(BF16)
            dq = mm(keys_t, d_scores).T.astype(BF16).astype(F32)
            dq_o[:, lanes] = (dq * score_scale).astype(BF16)
            dk_here = mm(d_scores, q_tile)
            dv_here = mm(rounded, d_tile)
            dk = dk_here if dk is None else dk + dk_here
            dv = dv_here if dv is None else dv + dv_here
        d_keys[group] = unpadded(dk, odd)
        d_values[group] = unpadded(dv, odd)
    for side, parts in ((0, d_keys), (kv_width, d_values)):
        for tile in range(groups // 2):
            lanes = slice(side + tile * LANES, side + (tile + 1) * LANES)
            total = (parts[2 * tile] + parts[2 * tile + 1]).astype(BF16).astype(F32)
            dmkv_o[:, lanes] = total[:slots]
            dkv_o[:, lanes] = total[slots:]
    out_o[...] = (seg[...].astype(F32) + mm(cr_o[...], wo[...])).astype(BF16)


def owner_back_kernel(
    dmkv, mem, p, call, stat, mem_own, u, wo, wk, wv, gain, r_o, dmb_o, dc_o, g0_o, vec_o, later_s,
    *, chain,
):
    rows, width = mem.shape
    own = rows // chain
    kv_width = wk.shape[1]
    dmb = dmkv[...].astype(BF16)
    dmb_o[...] = dmb
    dmn = mm_nt(dmb[:, :kv_width], wk[...]) + mm_nt(dmb[:, kv_width:], wv[...])
    inverse = stat[2][:, :1]
    keep = stat[1][:, :1]
    retain = stat[0][:, :1]
    memory = mem[...]
    vec_o[0:1, :] = jnp.sum(dmn * memory * inverse, axis=0, keepdims=True)
    scaled = dmn * gain[...]
    inner = jnp.sum(scaled * memory, axis=1, keepdims=True) * (1.0 / width)
    r = inverse * scaled - memory * (inverse * inverse * inverse * inner)
    r_o[...] = r.astype(BF16)
    start = jnp.concatenate([mem_own[...]] * chain, axis=0)
    q = jnp.sum(r * start, axis=1, keepdims=True)
    kept = keep * r
    g0 = kept[:own]
    for c in range(1, chain):
        g0 = g0 + kept[c * own : (c + 1) * own]
    g0_o[...] = g0
    turned = mm_nt(r.astype(BF16), wo[...])
    later = jnp.zeros((own, width), F32)
    later_q = jnp.zeros((own, 1), F32)
    q_parts = [None] * chain
    for c in reversed(range(chain)):
        at = slice(c * own, (c + 1) * own)
        later_s[at, :] = later
        q_parts[c] = later_q
        later = turned[at] + retain[at] * later
        later_q = q[at] + retain[at] * later_q
    ahead = later_s[...]
    context = call[...]
    d_retain = keep * jnp.concatenate(q_parts, axis=0) + jnp.sum(
        ahead * (p[...] - context), axis=1, keepdims=True
    )
    dz = d_retain * retain * (1.0 - retain)
    dc_o[...] = (1.0 - retain) * ahead + dz * u[...]
    v = jnp.sum(dz * context, axis=0, keepdims=True)
    vec_o[1:2, :] = v
    vec_o[2:3, :] = row_times(v, wo[...], False)


def finish_kernel(
    place, length, seg, xn, sn, s, kv, dc, dq, dkv_r, mem0, g0, wq, wk, wv, gain, vec,
    dkv_o, dqs_o, mem_o, vec_o,
):
    count, width = seg.shape
    slots = mem0.shape[0]
    kv_width = wk.shape[1]
    pairs = width // LANES
    groups = kv_width // HEAD
    allowed = lax.broadcasted_iota(jnp.int32, (count, slots), 0) < length[0, 0]
    d_keys = [None] * groups
    d_values = [None] * groups
    for group in range(groups):
        at, odd = (group // 2) * LANES, group % 2
        keys = padded(kv[:, at : at + LANES], odd)
        values = padded(kv[:, kv_width + at : kv_width + at + LANES], odd)
        keys_t = keys.T
        dk = dv = None
        for pair in range(group * pairs // groups, (group + 1) * pairs // groups):
            lanes = slice(pair * LANES, (pair + 1) * LANES)
            s_tile = s[:, lanes]
            weights = softmax_rows(mm_nt(keys, s_tile), allowed)
            d_tile = dc[:, lanes].astype(BF16)
            d_weights = mm_nt(values, d_tile).astype(BF16).astype(F32)
            d_scores = softmax_back(weights, d_weights).astype(BF16)
            dqs = mm(keys_t, d_scores).T.astype(BF16).astype(F32)
            dqs_o[:, lanes] = (dqs * score_scale).astype(BF16)
            dk_here = mm(d_scores, s_tile)
            dv_here = mm(weights.astype(BF16), d_tile)
            dk = dk_here if dk is None else dk + dk_here
            dv = dv_here if dv is None else dv + dv_here
        d_keys[group] = unpadded(dk, odd)
        d_values[group] = unpadded(dv, odd)
    for side, parts in ((0, d_keys), (kv_width, d_values)):
        for tile in range(groups // 2):
            lanes = slice(side + tile * LANES, side + (tile + 1) * LANES)
            total = (parts[2 * tile] + parts[2 * tile + 1]).astype(BF16).astype(F32)
            dkv_o[:, lanes] = (total + dkv_r[:, lanes]).astype(BF16)
    d_both = mm_nt(jnp.concatenate([dq[...], dqs_o[...]], axis=0), wq[...])
    dxn = d_both[:count] + mm_nt(dkv_o[:, :kv_width], wk[...]) + mm_nt(dkv_o[:, kv_width:], wv[...])
    dsn = d_both[count:]
    rows = seg[...].astype(F32)
    start = mem0[...].astype(F32)
    inverse = inverse_rms(start)
    gain_here = jnp.sum(dxn * (rows * inverse_rms(rows)), axis=0, keepdims=True) + jnp.sum(
        dsn * (start * inverse), axis=0, keepdims=True
    )
    vec_o[...] = jnp.zeros(vec_o.shape, F32)
    vec_o[0:1, :] = vec[0:1, :] + gain_here
    vec_o[1:3, :] = vec[1:3, :]
    scaled = dsn * gain[...]
    inner = jnp.sum(scaled * start, axis=1, keepdims=True) * (1.0 / width)
    d_start = inverse * scaled - start * (inverse * inverse * inverse * inner)
    own = g0.shape[0]
    held = jnp.concatenate([g0[...]] * (slots // own), axis=0)
    at = lax.broadcasted_iota(jnp.int32, (slots, 1), 0)
    first = place[0, 0] * own
    mem_o[...] = d_start + jnp.where((at >= first) & (at < first + own), held, 0.0)


def arranged(source, scratch, target, me, table):
    blocks, height, _ = scratch.shape
    for b in range(blocks):
        scratch[b] = source[b * height : (b + 1) * height]
    for b in range(blocks):
        target[b * height : (b + 1) * height, :] = scratch[me ^ table[b]]


def product_kernel(me, a1, a2, b1, b2, send_o, keep_o, scratch, lined, *, table):
    t1 = a1.shape[0]
    at = jnp.concatenate([a1[...].astype(F32).T, a2[...].astype(F32).T], axis=1)
    arranged(at, scratch, lined, me[0, 0], table)
    half = lined.shape[0] // 2
    right = jnp.concatenate([b1[...], b2[...]], axis=0)
    keep_o[...] = mm(lined[:half].astype(BF16), right)
    send_o[...] = mm(lined[half:].astype(BF16), right)


def vectors_kernel(me, mem, vec, send_o, keep_o, scratch, lined, *, table):
    fill = jnp.zeros((LANES - vec.shape[0], vec.shape[1]), F32)
    at = jnp.concatenate([mem[...].T, jnp.concatenate([vec[...], fill], axis=0).T], axis=1)
    arranged(at, scratch, lined, me[0, 0], table)
    half = lined.shape[0] // 2
    keep_o[...] = lined[:half]
    send_o[...] = lined[half:]


SMEM = pl.BlockSpec(memory_space=pltpu.SMEM)
VMEM = pl.BlockSpec(memory_space=pltpu.VMEM)


def call(kernel, scalars, arrays, outs, scratch=(), name=None):
    return pl.pallas_call(
        kernel,
        out_shape=tuple(jax.ShapeDtypeStruct(shape, kind) for shape, kind in outs),
        in_specs=[SMEM] * len(scalars) + [VMEM] * len(arrays),
        out_specs=tuple([VMEM] * len(outs)),
        scratch_shapes=[pltpu.VMEM(shape, kind) for shape, kind in scratch],
        name=name,
    )(*scalars, *arrays)


def per_device(
    chain,
    docs,
    segments,
    lengths,
    query_weight,
    key_weight,
    value_weight,
    out_weight,
    norm_gain,
    gate_vector,
    gate_bias,
    memory_init,
    cotangent,
):
    segment, cot = segments[0, 0], cotangent[0, 0]
    count, width = segment.shape
    slots = memory_init.shape[0]
    kv2 = 2 * key_weight.shape[1]
    own = slots // chain
    devices = chain * docs
    place = lax.axis_index("chain")
    me = (place * docs + lax.axis_index("dp")).reshape(1, 1)
    gain, vector = norm_gain[None, :], gate_vector[None, :]
    bias = jnp.tile(lax.dynamic_slice(gate_bias, (place * own,), (own,)), chain)[:, None]
    mem_own = lax.dynamic_slice(memory_init, (place * own, 0), (own, width)).astype(F32)

    def trade(blocks):
        return lax.all_to_all(blocks, "chain", 0, 0, tiled=True)

    xn, q, kv, sn, s, c, u = call(
        prepare_kernel,
        [lengths],
        [segment, query_weight, key_weight, value_weight, out_weight, gain, vector, memory_init],
        [
            ((count, width), BF16),
            ((count, width), BF16),
            ((count, kv2), BF16),
            ((slots, width), BF16),
            ((slots, width), BF16),
            ((slots, width), F32),
            ((1, width), F32),
        ],
        name="prepare",
    )
    c_all = trade(c)
    p, mem, stat, mn, mkv = call(
        functools.partial(owner_kernel, chain=chain),
        [],
        [c_all, bias, mem_own, u, out_weight, key_weight, value_weight, gain],
        [
            ((slots, width), F32),
            ((slots, width), F32),
            ((3, slots, LANES), F32),
            ((slots, width), BF16),
            ((slots, kv2), F32),
        ],
        name="owner",
    )
    mkv_here = trade(mkv)
    out, cr, d_out, dq, dkv_r, dmkv = call(
        read_kernel,
        [lengths],
        [segment, cot, q, kv, mkv_here, out_weight],
        [
            ((count, width), BF16),
            ((count, width), BF16),
            ((count, width), BF16),
            ((count, width), BF16),
            ((count, kv2), F32),
            ((slots, kv2), F32),
        ],
        [((count, width), BF16), ((8, LANES), F32)],
        name="read",
    )
    dmkv_all = trade(dmkv)
    r, dmb, dc, g0, vec = call(
        functools.partial(owner_back_kernel, chain=chain),
        [],
        [dmkv_all, mem, p, c_all, stat, mem_own, u, out_weight, key_weight, value_weight, gain],
        [
            ((slots, width), BF16),
            ((slots, kv2), BF16),
            ((slots, width), F32),
            ((own, width), F32),
            ((3, width), F32),
        ],
        [((slots, width), F32)],
        name="owner_back",
    )
    dc_here = trade(dc)
    dkv, dqs, d_mem, vec = call(
        finish_kernel,
        [place.reshape(1, 1), lengths],
        [
            segment, xn, sn, s, kv, dc_here, dq, dkv_r, memory_init, g0,
            query_weight, key_weight, value_weight, gain, vec,
        ],
        [((count, kv2), BF16), ((slots, width), BF16), ((slots, width), F32), ((8, width), F32)],
        name="finish",
    )

    bits = devices.bit_length() - 1
    low = docs.bit_length() - 1
    others = list(range(low + 1, bits))
    within = list(range(low))
    orders = [
        [low] + within + others,
        [low] + others + within,
        [low] + others[1:] + within + others[:1],
    ]
    height = width // devices

    def table_of(order):
        table = []
        for b in range(devices):
            table.append(sum(((b >> (bits - 1 - k)) & 1) << pos for k, pos in enumerate(order)))
        return tuple(table)

    def products(order, a1, a2, b1, b2, name):
        tokens = a1.shape[0] + a2.shape[0]
        half = ((width // 2, b1.shape[1]), F32)
        return call(
            functools.partial(product_kernel, table=table_of(order)),
            [me],
            [a1, a2, b1, b2],
            [half, half],
            [((devices, height, tokens), F32), ((width, tokens), F32)],
            name=name,
        )

    def swap(rows, pos):
        return lax.ppermute(
            rows, ("chain", "dp"), [(i, i ^ (1 << pos)) for i in range(devices)]
        )

    def scattered(order, send, keep):
        total = keep + swap(send, order[0])
        for pos in order[1:]:
            half = total.shape[0] // 2
            total = total[:half] + swap(total[half:], pos)
        return total

    g_out = scattered(orders[0], *products(orders[0], cr, p.astype(BF16), d_out, r, "out_product"))
    g_query = scattered(orders[1], *products(orders[1], xn, sn, dq, dqs, "query_product"))
    g_kv = scattered(orders[2], *products(orders[2], xn, mn, dkv, dmb, "kv_product"))
    half = ((width // 2, slots + LANES), F32)
    g_rest = scattered(
        orders[2],
        *call(
            functools.partial(vectors_kernel, table=table_of(orders[2])),
            [me],
            [d_mem, vec],
            [half, half],
            [((devices, height, slots + LANES), F32), ((width, slots + LANES), F32)],
            name="vectors",
        ),
    )
    g_out = g_out + g_rest[:, slots + 1 : slots + 2] * vector
    return (
        out[None, None],
        g_query,
        g_kv[:, : kv2 // 2],
        g_kv[:, kv2 // 2 :],
        g_out,
        g_rest[:, slots],
        g_rest[:, slots + 2],
        g_rest[:, :slots].T,
    )


def solution(mesh):
    in_specs = (
        P("dp", "chain", None, None),
        P("dp", "chain"),
        P(),
        P(),
        P(),
        P(),
        P(),
        P(),
        P(),
        P(),
        P("dp", "chain", None, None),
    )
    out_specs = (
        P("dp", "chain", None, None),
        P(("chain", "dp"), None),
        P(("chain", "dp"), None),
        P(("chain", "dp"), None),
        P(("chain", "dp"), None),
        P(("chain", "dp")),
        P(("chain", "dp")),
        P(None, ("chain", "dp")),
    )
    return jax.shard_map(
        functools.partial(per_device, mesh.shape["chain"], mesh.shape["dp"]),
        mesh=mesh,
        in_specs=in_specs,
        out_specs=out_specs,
        check_vma=False,
    )
```

```python
import functools

import jax
import jax.numpy as jnp
from jax import lax
from jax.experimental import pallas as pl
from jax.experimental.pallas import tpu as pltpu
from jax.sharding import PartitionSpec as P


HEAD = 64
LANES = 128
epsilon = 1e-05
score_scale = 0.125
F32 = jnp.float32
BF16 = jnp.bfloat16


def mm(a, b):
    return lax.dot_general(a, b, (((1,), (0,)), ((), ())), preferred_element_type=F32)


def mm_nt(a, b):
    return lax.dot_general(a, b, (((1,), (1,)), ((), ())), preferred_element_type=F32)


def inverse_rms(rows):
    return lax.rsqrt(jnp.mean(rows * rows, axis=-1, keepdims=True) + epsilon)


def low_lanes(shape):
    return lax.broadcasted_iota(jnp.int32, shape, 1) < HEAD


def padded(tile, odd):
    wide = tile.astype(F32)
    mine = low_lanes(wide.shape) != bool(odd)
    here = jnp.where(mine, wide, 0.0)
    there = pltpu.roll(here, HEAD, 1)
    low, high = (there, here) if odd else (here, there)
    return jnp.concatenate([low, high], axis=0).astype(BF16)


def unpadded(total, odd):
    rows = total.shape[0] // 2
    low_mask = low_lanes((rows, LANES))
    low = jnp.where(low_mask, total[:rows], 0.0)
    high = jnp.where(low_mask, 0.0, total[rows:])
    return high + pltpu.roll(low, HEAD, 1) if odd else low + pltpu.roll(high, HEAD, 1)


def softmax_rows(scores, allowed):
    width = scores.shape[0] // 2
    halves = []
    for part in (scores[:width], scores[width:]):
        part = jnp.where(allowed, part, -1e30)
        raised = jnp.exp(part - jnp.max(part, axis=0, keepdims=True))
        halves.append(raised / jnp.sum(raised, axis=0, keepdims=True))
    return jnp.concatenate(halves, axis=0)


def softmax_back(weights, d_weights):
    width = weights.shape[0] // 2
    halves = []
    for at in (0, width):
        w, d = weights[at : at + width], d_weights[at : at + width]
        halves.append(w * (d - jnp.sum(w * d, axis=0, keepdims=True)))
    return jnp.concatenate(halves, axis=0)


def split3(value):
    high = value.astype(BF16)
    rest = value - high.astype(F32)
    mid = rest.astype(BF16)
    return high, mid, (rest - mid.astype(F32)).astype(BF16)


def row_times(row, matrix, transposed):
    pieces = split3(row)
    stacked = jnp.concatenate(list(pieces) + [jnp.zeros_like(pieces[0])] * 13, axis=0)
    return jnp.sum((mm_nt if transposed else mm)(stacked, matrix), axis=0, keepdims=True)


def prepare_kernel(
    length, seg, wq, wk, wv, wo, gain, vector, mem0, xn_o, q_o, kv_o, sn_o, s_o, c_o, u_o
):
    count = seg.shape[0]
    kv_width = wk.shape[1]
    rows = seg[...].astype(F32)
    start = mem0[...].astype(F32)
    g = gain[...]
    xn = (rows * inverse_rms(rows) * g).astype(BF16)
    sn = (start * inverse_rms(start) * g).astype(BF16)
    xn_o[...] = xn
    sn_o[...] = sn
    both = mm(jnp.concatenate([xn, sn], axis=0), wq[...]) * score_scale
    q_o[...] = both[:count].astype(BF16)
    s_o[...] = both[count:].astype(BF16)
    kv_o[:, :kv_width] = mm(xn, wk[...]).astype(BF16)
    kv_o[:, kv_width:] = mm(xn, wv[...]).astype(BF16)
    u_o[...] = row_times(vector[...], wo[...], True)
    slots = mem0.shape[0]
    allowed = lax.broadcasted_iota(jnp.int32, (count, slots), 0) < length[0, 0]
    pairs = s_o.shape[1] // LANES
    groups = kv_width // HEAD
    for group in range(groups):
        at, odd = (group // 2) * LANES, group % 2
        keys = padded(kv_o[:, at : at + LANES], odd)
        values_t = padded(kv_o[:, kv_width + at : kv_width + at + LANES], odd).T
        for pair in range(group * pairs // groups, (group + 1) * pairs // groups):
            lanes = slice(pair * LANES, (pair + 1) * LANES)
            weights = softmax_rows(mm_nt(keys, s_o[:, lanes]), allowed).astype(BF16)
            c_o[:, lanes] = mm(values_t, weights).T.astype(BF16).astype(F32)


def owner_kernel(
    call, bias, mem_own, u, wo, wk, wv, gain, p_o, mem_o, stat_o, mn_o, mkv_o, *, chain
):
    rows = call.shape[0]
    own = rows // chain
    logits = jnp.sum(call[...] * u[...], axis=1, keepdims=True) + bias[...]
    retain = jax.nn.sigmoid(logits)
    stat_o[0] = jnp.broadcast_to(retain, (rows, LANES))
    memory = jnp.zeros((own, call.shape[1]), F32)
    keep = jnp.ones((own, LANES), F32)
    for c in range(chain):
        at = slice(c * own, (c + 1) * own)
        p_o[at, :] = memory
        stat_o[1, at, :] = keep
        ret = stat_o[0, at, :]
        memory = ret[:, :1] * memory + (1.0 - ret[:, :1]) * call[at, :]
        keep = keep * ret
    start = jnp.concatenate([mem_own[...]] * chain, axis=0)
    mem = stat_o[1][:, :1] * start + mm(p_o[...].astype(BF16), wo[...])
    mem_o[...] = mem
    inverse = inverse_rms(mem)
    stat_o[2] = jnp.broadcast_to(inverse, (rows, LANES))
    mn = (mem * inverse * gain[...]).astype(BF16)
    mn_o[...] = mn
    width = wk.shape[1]
    mkv_o[:, :width] = mm(mn, wk[...]).astype(BF16).astype(F32)
    mkv_o[:, width:] = mm(mn, wv[...]).astype(BF16).astype(F32)


def read_kernel(
    length, seg, cot, q, kv, mkv, wo, out_o, cr_o, do_o, dq_o, dkv_o, dmkv_o, dcr_s, w_s
):
    count, width = q.shape
    slots = mkv.shape[0]
    kv_width = kv.shape[1] // 2
    pairs = width // LANES
    groups = kv_width // HEAD
    valid = lax.broadcasted_iota(jnp.int32, (count, 1), 0) < length[0, 0]
    d_out = jnp.where(valid, cot[...].astype(F32), 0.0).astype(BF16)
    do_o[...] = d_out
    dcr_s[...] = mm_nt(d_out, wo[...]).astype(BF16)
    key_at = lax.broadcasted_iota(jnp.int32, (slots + count, count), 0) - slots
    query_at = lax.broadcasted_iota(jnp.int32, (slots + count, count), 1)
    allowed = (key_at < 0) | ((key_at <= query_at) & (key_at < length[0, 0]))
    d_keys = [None] * groups
    d_values = [None] * groups
    for group in range(groups):
        at, odd = (group // 2) * LANES, group % 2
        keys = padded(
            jnp.concatenate(
                [mkv[:, at : at + LANES], kv[:, at : at + LANES].astype(F32)], axis=0
            ),
            odd,
        )
        at_v = kv_width + at
        values = padded(
            jnp.concatenate(
                [mkv[:, at_v : at_v + LANES], kv[:, at_v : at_v + LANES].astype(F32)], axis=0
            ),
            odd,
        )
        keys_t, values_t = keys.T, values.T
        dk = dv = None
        for pair in range(group * pairs // groups, (group + 1) * pairs // groups):
            lanes = slice(pair * LANES, (pair + 1) * LANES)
            q_tile = q[:, lanes]
            weights = softmax_rows(mm_nt(keys, q_tile), allowed)
            rounded = weights.astype(BF16)
            cr_o[:, lanes] = mm(values_t, rounded).T.astype(BF16)
            d_tile = dcr_s[:, lanes]
            d_weights = mm_nt(values, d_tile).astype(BF16).astype(F32)
            d_scores = softmax_back(weights, d_weights).astype(BF16)
            dq = mm(keys_t, d_scores).T.astype(BF16).astype(F32)
            dq_o[:, lanes] = (dq * score_scale).astype(BF16)
            dk_here = mm(d_scores, q_tile)
            dv_here = mm(rounded, d_tile)
            dk = dk_here if dk is None else dk + dk_here
            dv = dv_here if dv is None else dv + dv_here
        d_keys[group] = unpadded(dk, odd)
        d_values[group] = unpadded(dv, odd)
    for side, parts in ((0, d_keys), (kv_width, d_values)):
        for tile in range(groups // 2):
            lanes = slice(side + tile * LANES, side + (tile + 1) * LANES)
            total = (parts[2 * tile] + parts[2 * tile + 1]).astype(BF16).astype(F32)
            dmkv_o[:, lanes] = total[:slots]
            dkv_o[:, lanes] = total[slots:]
    out_o[...] = (seg[...].astype(F32) + mm(cr_o[...], wo[...])).astype(BF16)


def owner_back_kernel(
    dmkv, mem, p, call, stat, mem_own, u, wo, wk, wv, gain, r_o, dmb_o, dc_o, g0_o, vec_o, later_s,
    *, chain,
):
    rows, width = mem.shape
    own = rows // chain
    kv_width = wk.shape[1]
    dmb = dmkv[...].astype(BF16)
    dmb_o[...] = dmb
    dmn = mm_nt(dmb[:, :kv_width], wk[...]) + mm_nt(dmb[:, kv_width:], wv[...])
    inverse = stat[2][:, :1]
    keep = stat[1][:, :1]
    retain = stat[0][:, :1]
    memory = mem[...]
    vec_o[0:1, :] = jnp.sum(dmn * memory * inverse, axis=0, keepdims=True)
    scaled = dmn * gain[...]
    inner = jnp.sum(scaled * memory, axis=1, keepdims=True) * (1.0 / width)
    r = inverse * scaled - memory * (inverse * inverse * inverse * inner)
    r_o[...] = r.astype(BF16)
    start = jnp.concatenate([mem_own[...]] * chain, axis=0)
    q = jnp.sum(r * start, axis=1, keepdims=True)
    kept = keep * r
    g0 = kept[:own]
    for c in range(1, chain):
        g0 = g0 + kept[c * own : (c + 1) * own]
    g0_o[...] = g0
    turned = mm_nt(r.astype(BF16), wo[...])
    later = jnp.zeros((own, width), F32)
    later_q = jnp.zeros((own, 1), F32)
    q_parts = [None] * chain
    for c in reversed(range(chain)):
        at = slice(c * own, (c + 1) * own)
        later_s[at, :] = later
        q_parts[c] = later_q
        later = turned[at] + retain[at] * later
        later_q = q[at] + retain[at] * later_q
    ahead = later_s[...]
    context = call[...]
    d_retain = keep * jnp.concatenate(q_parts, axis=0) + jnp.sum(
        ahead * (p[...] - context), axis=1, keepdims=True
    )
    dz = d_retain * retain * (1.0 - retain)
    dc_o[...] = (1.0 - retain) * ahead + dz * u[...]
    v = jnp.sum(dz * context, axis=0, keepdims=True)
    vec_o[1:2, :] = v
    vec_o[2:3, :] = row_times(v, wo[...], False)


def finish_kernel(
    place, length, seg, xn, sn, s, kv, dc, dq, dkv_r, mem0, g0, wq, wk, wv, gain, vec,
    dkv_o, dqs_o, mem_o, vec_o,
):
    count, width = seg.shape
    slots = mem0.shape[0]
    kv_width = wk.shape[1]
    pairs = width // LANES
    groups = kv_width // HEAD
    allowed = lax.broadcasted_iota(jnp.int32, (count, slots), 0) < length[0, 0]
    d_keys = [None] * groups
    d_values = [None] * groups
    for group in range(groups):
        at, odd = (group // 2) * LANES, group % 2
        keys = padded(kv[:, at : at + LANES], odd)
        values = padded(kv[:, kv_width + at : kv_width + at + LANES], odd)
        keys_t = keys.T
        dk = dv = None
        for pair in range(group * pairs // groups, (group + 1) * pairs // groups):
            lanes = slice(pair * LANES, (pair + 1) * LANES)
            s_tile = s[:, lanes]
            weights = softmax_rows(mm_nt(keys, s_tile), allowed)
            d_tile = dc[:, lanes].astype(BF16)
            d_weights = mm_nt(values, d_tile).astype(BF16).astype(F32)
            d_scores = softmax_back(weights, d_weights).astype(BF16)
            dqs = mm(keys_t, d_scores).T.astype(BF16).astype(F32)
            dqs_o[:, lanes] = (dqs * score_scale).astype(BF16)
            dk_here = mm(d_scores, s_tile)
            dv_here = mm(weights.astype(BF16), d_tile)
            dk = dk_here if dk is None else dk + dk_here
            dv = dv_here if dv is None else dv + dv_here
        d_keys[group] = unpadded(dk, odd)
        d_values[group] = unpadded(dv, odd)
    for side, parts in ((0, d_keys), (kv_width, d_values)):
        for tile in range(groups // 2):
            lanes = slice(side + tile * LANES, side + (tile + 1) * LANES)
            total = (parts[2 * tile] + parts[2 * tile + 1]).astype(BF16).astype(F32)
            dkv_o[:, lanes] = (total + dkv_r[:, lanes]).astype(BF16)
    d_both = mm_nt(jnp.concatenate([dq[...], dqs_o[...]], axis=0), wq[...])
    dxn = d_both[:count] + mm_nt(dkv_o[:, :kv_width], wk[...]) + mm_nt(dkv_o[:, kv_width:], wv[...])
    dsn = d_both[count:]
    rows = seg[...].astype(F32)
    start = mem0[...].astype(F32)
    inverse = inverse_rms(start)
    gain_here = jnp.sum(dxn * (rows * inverse_rms(rows)), axis=0, keepdims=True) + jnp.sum(
        dsn * (start * inverse), axis=0, keepdims=True
    )
    vec_o[...] = jnp.zeros(vec_o.shape, F32)
    vec_o[0:1, :] = vec[0:1, :] + gain_here
    vec_o[1:3, :] = vec[1:3, :]
    scaled = dsn * gain[...]
    inner = jnp.sum(scaled * start, axis=1, keepdims=True) * (1.0 / width)
    d_start = inverse * scaled - start * (inverse * inverse * inverse * inner)
    own = g0.shape[0]
    held = jnp.concatenate([g0[...]] * (slots // own), axis=0)
    at = lax.broadcasted_iota(jnp.int32, (slots, 1), 0)
    first = place[0, 0] * own
    mem_o[...] = d_start + jnp.where((at >= first) & (at < first + own), held, 0.0)


def arranged(source, scratch, lined, me, table):
    blocks, height, _ = scratch.shape
    tall = source.shape[1]
    for b in range(blocks):
        scratch[b, :, :tall] = source[b * height : (b + 1) * height]
    for b in range(blocks):
        lined[b * height : (b + 1) * height, :tall] = scratch[me ^ table[b], :, :tall]


def product_kernel(me, *refs, plan):
    ins = refs[: plan["ins"]]
    outs = refs[plan["ins"] : plan["ins"] + 2 * len(plan["groups"])]
    scratch, lined = refs[-2:]
    half = lined.shape[0] // 2
    for index, (columns, lefts, rights, passed, table) in enumerate(plan["groups"]):
        sources = [ins[i][...].astype(F32) for i in (*lefts, *passed)]
        tokens = sum(ins[i].shape[0] for i in lefts)
        tall = sum(part.shape[0] for part in sources)
        arranged(jnp.concatenate(sources, axis=0).T, scratch, lined, me[0, 0], table)
        right = jnp.concatenate([ins[i][:, columns[0] : columns[1]] for i in rights], axis=0)
        for side, out in ((0, outs[2 * index]), (half, outs[2 * index + 1])):
            left = lined[side : side + half, :tokens].astype(BF16)
            out[:, : right.shape[1]] = mm(left, right)
            if passed:
                out[:, right.shape[1] :] = lined[side : side + half, tokens:tall]


SMEM = pl.BlockSpec(memory_space=pltpu.SMEM)
VMEM = pl.BlockSpec(memory_space=pltpu.VMEM)


def call(kernel, scalars, arrays, outs, scratch=()):
    return pl.pallas_call(
        kernel,
        out_shape=tuple(jax.ShapeDtypeStruct(shape, kind) for shape, kind in outs),
        in_specs=[SMEM] * len(scalars) + [VMEM] * len(arrays),
        out_specs=tuple([VMEM] * len(outs)),
        scratch_shapes=[pltpu.VMEM(shape, kind) for shape, kind in scratch],
    )(*scalars, *arrays)


def per_device(
    chain,
    docs,
    segments,
    lengths,
    query_weight,
    key_weight,
    value_weight,
    out_weight,
    norm_gain,
    gate_vector,
    gate_bias,
    memory_init,
    cotangent,
):
    segment, cot = segments[0, 0], cotangent[0, 0]
    count, width = segment.shape
    slots = memory_init.shape[0]
    kv2 = 2 * key_weight.shape[1]
    own = slots // chain
    devices = chain * docs
    place = lax.axis_index("chain")
    me = (place * docs + lax.axis_index("dp")).reshape(1, 1)
    gain, vector = norm_gain[None, :], gate_vector[None, :]
    bias = jnp.tile(lax.dynamic_slice(gate_bias, (place * own,), (own,)), chain)[:, None]
    mem_own = lax.dynamic_slice(memory_init, (place * own, 0), (own, width)).astype(F32)

    bits = devices.bit_length() - 1
    low = docs.bit_length() - 1
    others = list(range(low + 1, bits))
    within = list(range(low))
    order_a = [low] + within + others
    order_b = [low] + others[:1] + within + others[1:]
    order_c = [low] + others[1:] + others[:1] + within
    meet = low + 2
    cut = width * 5 // 8 // LANES * LANES
    height = width // devices

    def table_of(order):
        table = []
        for b in range(devices):
            table.append(sum(((b >> (bits - 1 - k)) & 1) << pos for k, pos in enumerate(order)))
        return tuple(table)

    def products(arrays, groups):
        outs, most, plan = [], 0, []
        for columns, lefts, rights, passed, order in groups:
            extra = sum(arrays[i].shape[0] for i in passed)
            shape = (width // 2, columns[1] - columns[0] + extra)
            outs += [(shape, F32), (shape, F32)]
            most = max(most, extra + sum(arrays[i].shape[0] for i in lefts))
            plan.append((columns, lefts, rights, passed, table_of(order)))
        return call(
            functools.partial(product_kernel, plan={"ins": len(arrays), "groups": plan}),
            [me],
            arrays,
            outs,
            [((devices, height, most), F32), ((width, most), F32)],
        )

    def swap(rows, pos):
        return lax.ppermute(rows, ("chain", "dp"), [(i, i ^ (1 << pos)) for i in range(devices)])

    def halved(total, order):
        for pos in order:
            half = total.shape[0] // 2
            total = total[:half] + swap(total[half:], pos)
        return total

    def scattered(kept, sent, order):
        return halved(kept + swap(sent, order[0]), order[1:])

    def trade(blocks):
        return lax.all_to_all(blocks, "chain", 0, 0, tiled=True)

    xn, q, kv, sn, s, c, u = call(
        prepare_kernel,
        [lengths],
        [segment, query_weight, key_weight, value_weight, out_weight, gain, vector, memory_init],
        [
            ((count, width), BF16),
            ((count, width), BF16),
            ((count, kv2), BF16),
            ((slots, width), BF16),
            ((slots, width), BF16),
            ((slots, width), F32),
            ((1, width), F32),
        ],
    )
    c_all = trade(c)
    p, mem, stat, mn, mkv = call(
        functools.partial(owner_kernel, chain=chain),
        [],
        [c_all, bias, mem_own, u, out_weight, key_weight, value_weight, gain],
        [
            ((slots, width), F32),
            ((slots, width), F32),
            ((3, slots, LANES), F32),
            ((slots, width), BF16),
            ((slots, kv2), F32),
        ],
    )
    mkv_here = trade(mkv)
    out, cr, d_out, dq, dkv_r, dmkv = call(
        read_kernel,
        [lengths],
        [segment, cot, q, kv, mkv_here, out_weight],
        [
            ((count, width), BF16),
            ((count, width), BF16),
            ((count, width), BF16),
            ((count, width), BF16),
            ((count, kv2), F32),
            ((slots, kv2), F32),
        ],
        [((count, width), BF16), ((8, LANES), F32)],
    )
    dmkv_all = trade(dmkv)
    early_a, sent_a, early_b, sent_b = products(
        [xn, dq], [((0, cut), (0,), (1,), (), order_a), ((cut, width), (0,), (1,), (), order_b)]
    )
    early_a = scattered(early_a, sent_a, order_a[:meet])
    early_b = scattered(early_b, sent_b, order_b[:meet])
    r, dmb, dc, g0, vec = call(
        functools.partial(owner_back_kernel, chain=chain),
        [],
        [dmkv_all, mem, p, c_all, stat, mem_own, u, out_weight, key_weight, value_weight, gain],
        [
            ((slots, width), BF16),
            ((slots, kv2), BF16),
            ((slots, width), F32),
            ((own, width), F32),
            ((3, width), F32),
        ],
        [((slots, width), F32)],
    )
    dc_here = trade(dc)
    out_a, sent_a, out_b, sent_b = products(
        [cr, p, d_out, r],
        [
            ((0, width // 2), (0, 1), (2, 3), (), order_a),
            ((width // 2, width), (0, 1), (2, 3), (), order_b),
        ],
    )
    out_a = scattered(out_a, sent_a, order_a[:meet])
    out_b = scattered(out_b, sent_b, order_b[:meet])
    dkv, dqs, d_mem, vec = call(
        finish_kernel,
        [place.reshape(1, 1), lengths],
        [
            segment, xn, sn, s, kv, dc_here, dq, dkv_r, memory_init, g0,
            query_weight, key_weight, value_weight, gain, vec,
        ],
        [
            ((count, kv2), BF16),
            ((slots, width), BF16),
            ((slots, width), F32),
            ((LANES, width), F32),
        ],
    )
    late_a, sent_a, late_b, sent_b, late_c, sent_c = products(
        [sn, dqs, xn, mn, dkv, dmb, d_mem, vec],
        [
            ((0, cut), (0,), (1,), (), order_a),
            ((cut, width), (0,), (1,), (6, 7), order_b),
            ((0, kv2), (2, 3), (4, 5), (), order_c),
        ],
    )
    late_a = scattered(late_a, sent_a, order_a[:meet])
    late_b = scattered(late_b, sent_b, order_b[:meet])
    g_kv = scattered(late_c, sent_c, order_c)
    right = width - cut
    joined = jnp.concatenate(
        [late_a + early_a, late_b[:, :right] + early_b, late_b[:, right:], out_a, out_b], axis=1
    )
    joined = halved(joined, order_a[meet:])
    extra = joined[:, width : width + slots + LANES]
    g_out = joined[:, width + slots + LANES :] + extra[:, slots + 1 : slots + 2] * vector
    return (
        out[None, None],
        joined[:, :width],
        g_kv[:, : kv2 // 2],
        g_kv[:, kv2 // 2 :],
        g_out,
        extra[:, slots],
        extra[:, slots + 2],
        extra[:, :slots].T,
    )


def solution(mesh):
    in_specs = (
        P("dp", "chain", None, None),
        P("dp", "chain"),
        P(),
        P(),
        P(),
        P(),
        P(),
        P(),
        P(),
        P(),
        P("dp", "chain", None, None),
    )
    out_specs = (
        P("dp", "chain", None, None),
        P(("chain", "dp"), None),
        P(("chain", "dp"), None),
        P(("chain", "dp"), None),
        P(("chain", "dp"), None),
        P(("chain", "dp")),
        P(("chain", "dp")),
        P(None, ("chain", "dp")),
    )

    def step(*args):
        return per_device(mesh.shape["chain"], mesh.shape["dp"], *args)

    return jax.shard_map(
        step, mesh=mesh, in_specs=in_specs, out_specs=out_specs, check_vma=False
    )
```

```python
import functools

import jax
import jax.numpy as jnp
from jax import lax
from jax.experimental import pallas as pl
from jax.experimental.pallas import tpu as pltpu
from jax.sharding import PartitionSpec as P


HEAD = 64
LANES = 128
epsilon = 1e-05
score_scale = 0.125
F32 = jnp.float32
BF16 = jnp.bfloat16


def mm(a, b):
    return lax.dot_general(a, b, (((1,), (0,)), ((), ())), preferred_element_type=F32)


def mm_nt(a, b):
    return lax.dot_general(a, b, (((1,), (1,)), ((), ())), preferred_element_type=F32)


def inverse_rms(rows):
    return lax.rsqrt(jnp.mean(rows * rows, axis=-1, keepdims=True) + epsilon)


def low_lanes(shape):
    return lax.broadcasted_iota(jnp.int32, shape, 1) < HEAD


def padded(tile, odd):
    wide = tile.astype(F32)
    mine = low_lanes(wide.shape) != bool(odd)
    here = jnp.where(mine, wide, 0.0)
    there = pltpu.roll(here, HEAD, 1)
    low, high = (there, here) if odd else (here, there)
    return jnp.concatenate([low, high], axis=0).astype(BF16)


def unpadded(total, odd):
    rows = total.shape[0] // 2
    low_mask = low_lanes((rows, LANES))
    low = jnp.where(low_mask, total[:rows], 0.0)
    high = jnp.where(low_mask, 0.0, total[rows:])
    return high + pltpu.roll(low, HEAD, 1) if odd else low + pltpu.roll(high, HEAD, 1)


def softmax_rows(scores, allowed):
    width = scores.shape[0] // 2
    halves = []
    for part in (scores[:width], scores[width:]):
        part = jnp.where(allowed, part, -1e30)
        raised = jnp.exp(part - jnp.max(part, axis=0, keepdims=True))
        halves.append(raised / jnp.sum(raised, axis=0, keepdims=True))
    return jnp.concatenate(halves, axis=0)


def softmax_back(weights, d_weights):
    width = weights.shape[0] // 2
    halves = []
    for at in (0, width):
        w, d = weights[at : at + width], d_weights[at : at + width]
        halves.append(w * (d - jnp.sum(w * d, axis=0, keepdims=True)))
    return jnp.concatenate(halves, axis=0)


def split3(value):
    high = value.astype(BF16)
    rest = value - high.astype(F32)
    mid = rest.astype(BF16)
    return high, mid, (rest - mid.astype(F32)).astype(BF16)


def row_times(row, matrix, transposed):
    pieces = split3(row)
    stacked = jnp.concatenate(list(pieces) + [jnp.zeros_like(pieces[0])] * 13, axis=0)
    return jnp.sum((mm_nt if transposed else mm)(stacked, matrix), axis=0, keepdims=True)


def prepare_kernel(
    length, seg, cot, wq, wk, wv, wo, gain, vector, mem0,
    q_o, kv_o, sn_o, s_o, c_o, u_o, both_o,
):
    count = seg.shape[0]
    kv_width = wk.shape[1]
    rows = seg[...].astype(F32)
    start = mem0[...].astype(F32)
    g = gain[...]
    xn = (rows * inverse_rms(rows) * g).astype(BF16)
    sn = (start * inverse_rms(start) * g).astype(BF16)
    sn_o[...] = sn
    both = mm(jnp.concatenate([xn, sn], axis=0), wq[...]) * score_scale
    q_o[...] = both[:count].astype(BF16)
    s_o[...] = both[count:].astype(BF16)
    kv_o[:, :kv_width] = mm(xn, wk[...]).astype(BF16)
    kv_o[:, kv_width:] = mm(xn, wv[...]).astype(BF16)
    u_o[...] = row_times(vector[...], wo[...], True)
    slots = mem0.shape[0]
    allowed = lax.broadcasted_iota(jnp.int32, (count, slots), 0) < length[0, 0]
    pairs = s_o.shape[1] // LANES
    groups = kv_width // HEAD
    for group in range(groups):
        at, odd = (group // 2) * LANES, group % 2
        keys = padded(kv_o[:, at : at + LANES], odd)
        values_t = padded(kv_o[:, kv_width + at : kv_width + at + LANES], odd).T
        for pair in range(group * pairs // groups, (group + 1) * pairs // groups):
            lanes = slice(pair * LANES, (pair + 1) * LANES)
            weights = softmax_rows(mm_nt(keys, s_o[:, lanes]), allowed).astype(BF16)
            c_o[:, lanes] = mm(values_t, weights).T.astype(BF16).astype(F32)
    valid = lax.broadcasted_iota(jnp.int32, (count, 1), 0) < length[0, 0]
    both_o[:count] = xn.astype(F32)
    both_o[count:] = jnp.where(valid, cot[...].astype(F32), 0.0)


def tiled(rows, times):
    return jnp.concatenate([rows] * times, axis=0)


def owner_scan_kernel(call, bias, u, p_o, stat_o, end_o, *, count):
    rows, width = call.shape
    own = rows // count
    logits = jnp.sum(call[...] * u[...], axis=1, keepdims=True) + tiled(bias[...], count)
    stat_o[0] = jnp.broadcast_to(jax.nn.sigmoid(logits), (rows, LANES))
    memory = jnp.zeros((own, width), F32)
    keep = jnp.ones((own, LANES), F32)
    for c in range(count):
        at = slice(c * own, (c + 1) * own)
        p_o[at, :] = memory
        stat_o[1, at, :] = keep
        ret = stat_o[0, at, :]
        memory = ret[:, :1] * memory + (1.0 - ret[:, :1]) * call[at, :]
        keep = keep * ret
    end_o[:, :width] = memory
    end_o[:, width:] = 1.0 - keep


def owner_kernel(
    p_in, stat, handed, mem_own, wo, wk, wv, gain, both_o, mem_o, stat_o, mkv_o, *, count
):
    rows, width = p_in.shape
    keep_here = stat[1]
    p = p_in[...] + keep_here[:, :1] * tiled(handed[:, :width], count)
    keep = keep_here * tiled(1.0 - handed[:, width:], count)
    both_o[rows:] = p
    mem = keep[:, :1] * tiled(mem_own[...], count) + mm(p.astype(BF16), wo[...])
    mem_o[...] = mem
    inverse = inverse_rms(mem)
    stat_o[0] = keep
    stat_o[1] = jnp.broadcast_to(inverse, (rows, LANES))
    mn = (mem * inverse * gain[...]).astype(BF16)
    both_o[:rows] = mn.astype(F32)
    kv_width = wk.shape[1]
    mkv_o[:, :kv_width] = mm(mn, wk[...]).astype(BF16).astype(F32)
    mkv_o[:, kv_width:] = mm(mn, wv[...]).astype(BF16).astype(F32)


def read_kernel(
    length, seg, cot, q, kv, mkv, wo, out_o, cr_o, dq_o, dkv_o, dmkv_o, dcr_s, cr_s
):
    count, width = q.shape
    slots = mkv.shape[0]
    kv_width = kv.shape[1] // 2
    pairs = width // LANES
    groups = kv_width // HEAD
    valid = lax.broadcasted_iota(jnp.int32, (count, 1), 0) < length[0, 0]
    d_out = jnp.where(valid, cot[...].astype(F32), 0.0).astype(BF16)
    dcr_s[...] = mm_nt(d_out, wo[...]).astype(BF16)
    key_at = lax.broadcasted_iota(jnp.int32, (slots + count, count), 0) - slots
    query_at = lax.broadcasted_iota(jnp.int32, (slots + count, count), 1)
    allowed = (key_at < 0) | ((key_at <= query_at) & (key_at < length[0, 0]))
    d_keys = [None] * groups
    d_values = [None] * groups
    for group in range(groups):
        at, odd = (group // 2) * LANES, group % 2
        keys = padded(
            jnp.concatenate(
                [mkv[:, at : at + LANES], kv[:, at : at + LANES].astype(F32)], axis=0
            ),
            odd,
        )
        at_v = kv_width + at
        values = padded(
            jnp.concatenate(
                [mkv[:, at_v : at_v + LANES], kv[:, at_v : at_v + LANES].astype(F32)], axis=0
            ),
            odd,
        )
        keys_t, values_t = keys.T, values.T
        dk = dv = None
        for pair in range(group * pairs // groups, (group + 1) * pairs // groups):
            lanes = slice(pair * LANES, (pair + 1) * LANES)
            q_tile = q[:, lanes]
            weights = softmax_rows(mm_nt(keys, q_tile), allowed)
            rounded = weights.astype(BF16)
            context = mm(values_t, rounded).T.astype(BF16)
            cr_s[:, lanes] = context
            cr_o[:, lanes] = context.astype(F32)
            d_tile = dcr_s[:, lanes]
            d_weights = mm_nt(values, d_tile).astype(BF16).astype(F32)
            d_scores = softmax_back(weights, d_weights).astype(BF16)
            dq = mm(keys_t, d_scores).T.astype(BF16).astype(F32)
            dq_o[:, lanes] = dq * score_scale
            dk_here = mm(d_scores, q_tile)
            dv_here = mm(rounded, d_tile)
            dk = dk_here if dk is None else dk + dk_here
            dv = dv_here if dv is None else dv + dv_here
        d_keys[group] = unpadded(dk, odd)
        d_values[group] = unpadded(dv, odd)
    for side, parts in ((0, d_keys), (kv_width, d_values)):
        for tile in range(groups // 2):
            lanes = slice(side + tile * LANES, side + (tile + 1) * LANES)
            total = (parts[2 * tile] + parts[2 * tile + 1]).astype(BF16).astype(F32)
            dmkv_o[:, lanes] = total[:slots]
            dkv_o[:, lanes] = total[slots:]
    out_o[...] = (seg[...].astype(F32) + mm(cr_s[...], wo[...])).astype(BF16)


def back_scan_kernel(
    place, dmkv, mem, ret, stat, mem_own, wo, wk, wv, gain,
    r_o, later_o, stat_o, end_o, g0_o, gain_o, *, count,
):
    rows, width = mem.shape
    own = rows // count
    kv_width = wk.shape[1]
    dmb = dmkv[...].astype(BF16)
    dmn = mm_nt(dmb[:, :kv_width], wk[...]) + mm_nt(dmb[:, kv_width:], wv[...])
    inverse = stat[1][:, :1]
    keep = stat[0][:, :1]
    memory = mem[...]
    gain_o[...] = jnp.sum(dmn * memory * inverse, axis=0, keepdims=True)
    scaled = dmn * gain[...]
    inner = jnp.sum(scaled * memory, axis=1, keepdims=True) * (1.0 / width)
    r = inverse * scaled - memory * (inverse * inverse * inverse * inner)
    rounded = r.astype(BF16)
    r_o[...] = rounded.astype(F32)
    q = jnp.sum(r * tiled(mem_own[...], count), axis=1, keepdims=True)
    kept = keep * r
    g0 = kept[:own]
    for c in range(1, count):
        g0 = g0 + kept[c * own : (c + 1) * own]
    at = lax.broadcasted_iota(jnp.int32, (rows, 1), 0)
    first = place[0, 0] * own
    g0_o[...] = jnp.where((at >= first) & (at < first + own), tiled(g0, count), 0.0)
    turned = mm_nt(rounded, wo[...])
    q = jnp.broadcast_to(q, (rows, LANES))
    later = jnp.zeros((own, width), F32)
    later_q = jnp.zeros((own, LANES), F32)
    passed = jnp.ones((own, LANES), F32)
    for c in reversed(range(count)):
        at = slice(c * own, (c + 1) * own)
        retain = ret[0, at, :]
        later_o[at, :] = later
        stat_o[0, at, :] = later_q
        stat_o[1, at, :] = passed
        later = turned[at] + retain[:, :1] * later
        later_q = q[at] + retain * later_q
        passed = passed * retain
    end_o[:, :width] = later
    end_o[:, width:] = later_q


def back_kernel(later, stat_b, handed, both, call, ret, stat, u, wo, gain_g, dc_o, vec_o, *, count):
    rows, width = later.shape
    passed = stat_b[1][:, :1]
    ahead = later[...] + passed * tiled(handed[:, :width], count)
    ahead_q = stat_b[0][:, :1] + passed * tiled(handed[:, width : width + 1], count)
    context = call[...]
    retain = ret[0][:, :1]
    d_retain = stat[0][:, :1] * ahead_q + jnp.sum(
        ahead * (both[rows:] - context), axis=1, keepdims=True
    )
    dz = d_retain * retain * (1.0 - retain)
    dc_o[...] = (1.0 - retain) * ahead + dz * u[...]
    v = jnp.sum(dz * context, axis=0, keepdims=True)
    vec_o[0:1, :] = gain_g[...]
    vec_o[1:2, :] = v
    vec_o[2:3, :] = row_times(v, wo[...], False)


def finish_kernel(
    key, length, seg, s, kv, dc, dq, dkv_r, wq, wk, wv, vec,
    dkv_o, keep_o, send_o, dqs_s, dkv_s,
):
    count, width = seg.shape
    slots = s.shape[0]
    pieces, piece, _ = dqs_s.shape
    kv_width = wk.shape[1]
    pairs = width // LANES
    groups = kv_width // HEAD
    allowed = lax.broadcasted_iota(jnp.int32, (count, slots), 0) < length[0, 0]
    d_keys = [None] * groups
    d_values = [None] * groups
    for group in range(groups):
        at, odd = (group // 2) * LANES, group % 2
        keys = padded(kv[:, at : at + LANES], odd)
        values = padded(kv[:, kv_width + at : kv_width + at + LANES], odd)
        keys_t = keys.T
        dk = dv = None
        for pair in range(group * pairs // groups, (group + 1) * pairs // groups):
            lanes = slice(pair * LANES, (pair + 1) * LANES)
            s_tile = s[:, lanes]
            weights = softmax_rows(mm_nt(keys, s_tile), allowed)
            d_tile = dc[:, lanes].astype(BF16)
            d_weights = mm_nt(values, d_tile).astype(BF16).astype(F32)
            d_scores = softmax_back(weights, d_weights).astype(BF16)
            dqs = mm(keys_t, d_scores).T.astype(BF16).astype(F32)
            dqs = dqs * score_scale
            for t in range(pieces):
                dqs_s[t, :, lanes] = dqs[t * piece : (t + 1) * piece]
            dk_here = mm(d_scores, s_tile)
            dv_here = mm(weights.astype(BF16), d_tile)
            dk = dk_here if dk is None else dk + dk_here
            dv = dv_here if dv is None else dv + dv_here
        d_keys[group] = unpadded(dk, odd)
        d_values[group] = unpadded(dv, odd)
    for side, parts in ((0, d_keys), (kv_width, d_values)):
        for tile in range(groups // 2):
            lanes = slice(side + tile * LANES, side + (tile + 1) * LANES)
            total = (parts[2 * tile] + parts[2 * tile + 1]).astype(BF16).astype(F32)
            total = (total + dkv_r[:, lanes]).astype(BF16)
            dkv_s[:, lanes] = total
            dkv_o[:, lanes] = total.astype(F32)
    dxn = mm_nt(dq[...].astype(BF16), wq[...])
    dxn = dxn + mm_nt(dkv_s[:, :kv_width], wk[...]) + mm_nt(dkv_s[:, kv_width:], wv[...])
    rows = seg[...].astype(F32)
    gain_here = jnp.sum(dxn * (rows * inverse_rms(rows)), axis=0, keepdims=True)
    half = slots // 2
    for t in range(pieces // 2):
        at = slice(t * piece, (t + 1) * piece)
        keep_o[at, :] = dqs_s[key[0, 0] ^ t]
        send_o[at, :] = dqs_s[key[0, 0] ^ (t + pieces // 2)]
    sums = jnp.concatenate(
        [vec[0:1, :] + gain_here, vec[1:3, :], jnp.zeros((5, width), F32)], axis=0
    )
    keep_o[half:] = sums
    send_o[half:] = sums


def last_kernel(
    key, me, near, far, total, sn, wq, mem0, gain, vector, kept, got, kept_out, got_out,
    query_o, out_o, small_o, mem_o, dqs_s, turn_s,
):
    slots, width = sn.shape
    pieces, piece, _ = dqs_s.shape
    height = kept.shape[0]
    for t in range(pieces // 2):
        at = slice(t * piece, (t + 1) * piece)
        dqs_s[key[0, 0] ^ t] = near[at]
        dqs_s[key[0, 0] ^ (t + pieces // 2)] = far[at]
    d_slots = jnp.concatenate([dqs_s[t] for t in range(pieces)], axis=0).astype(BF16)
    turned = sn[...].astype(F32).T
    for b in range(width // height):
        turn_s[b, :, :slots] = turned[b * height : (b + 1) * height]
    rows = turn_s[me[0, 0], :, :slots].astype(BF16)
    query_o[...] = kept[...] + got[...] + mm(rows, d_slots)
    dsn = mm_nt(d_slots, wq[...])
    start = mem0[...].astype(F32)
    inverse = inverse_rms(start)
    gain_row = jnp.sum(dsn * (start * inverse), axis=0, keepdims=True)
    scaled = dsn * gain[...]
    inner = jnp.sum(scaled * start, axis=1, keepdims=True) * (1.0 / width)
    d_start = inverse * scaled - start * (inverse * inverse * inverse * inner)
    sums = total[total.shape[0] - 8 :]
    small = jnp.concatenate(
        [sums, sums[0:1] + gain_row, jnp.zeros((slots - 9, width), F32)], axis=0
    )
    columns = jnp.concatenate([d_start, small], axis=0).T
    for b in range(width // height):
        turn_s[b] = columns[b * height : (b + 1) * height]
    mine = turn_s[me[0, 0]]
    held = kept_out[:, width:] + got_out[:, width:]
    mem_o[...] = (mine[:, :slots] + held).T
    small_o[...] = mine[:, slots:].T[:16]
    out_o[...] = (
        kept_out[:, :width]
        + got_out[:, :width]
        + mine[:, slots + 1 : slots + 2] * vector[...]
    )


def line_kernel(me, *refs, table, ranges):
    ins, out, turned = refs[:-2], refs[-2], refs[-1]
    blocks, height, _ = turned.shape
    lane = 0
    for i, first, last in ranges:
        across = slice(lane, lane + last - first)
        tall = ins[i][first:last].T
        for b in range(blocks):
            turned[b, :, across] = tall[b * height : (b + 1) * height]
        lane += last - first
    for b in range(blocks // 2):
        out[b * height : (b + 1) * height, :] = turned[me[0, 0] ^ table[b]].astype(BF16)


def product_kernel(me, *refs, plan):
    ins = refs[: plan["ins"]]
    outs = refs[plan["ins"] : plan["ins"] + 2 * len(plan["groups"])]
    turned, lined = refs[-2:]
    blocks, height, _ = turned.shape
    kind = turned.dtype
    places, lane = {}, 0
    for _, items in plan["groups"]:
        for lefts, _, _ in items:
            for left in lefts:
                if left in places:
                    continue
                if left[0] == "line":
                    places[left] = (ins[left[1]], slice(left[2], left[3]))
                    continue
                i, first, last = left
                rows = ins[i][first:last].astype(kind)
                across = slice(lane, lane + last - first)
                places[left] = (lined, across)
                tall = rows.T
                for b in range(blocks):
                    turned[b, :, across] = tall[b * height : (b + 1) * height]
                lane += last - first
    base = plan["groups"][0][0]
    for b in range(blocks // 2 if lane else 0):
        lined[b * height : (b + 1) * height, :lane] = turned[me[0, 0] ^ base[b], :, :lane]
    where = {dest: b for b, dest in enumerate(base)}
    for index, (table, items) in enumerate(plan["groups"]):
        runs = []
        for dest in table:
            b = where[dest]
            if runs and runs[-1][1] == b:
                runs[-1][1] = b + 1
            else:
                runs.append([b, b + 1])
        offset = 0
        cuts = []
        for lo, hi in runs:
            while lo < hi:
                take = min(hi - lo, blocks // 4 - offset % (blocks // 4))
                cuts.append((offset, lo, lo + take))
                offset += take
                lo += take
        at = 0
        for lefts, rights, columns in items:
            if rights:
                right = jnp.concatenate(
                    [
                        ins[i][first:last, columns[0] : columns[1]].astype(BF16)
                        for i, first, last in rights
                    ],
                    axis=0,
                )
            for offset, lo, hi in cuts:
                out = outs[2 * index + offset // (blocks // 4)]
                first = offset % (blocks // 4) * height
                to = slice(first, first + (hi - lo) * height)
                left = [
                    places[part][0][lo * height : hi * height, places[part][1]] for part in lefts
                ]
                if rights:
                    left = jnp.concatenate([part.astype(BF16) for part in left], axis=1)
                    out[to, at : at + right.shape[1]] = mm(left, right)
                else:
                    out[to, at : at + left[0].shape[1]] = sum(left[1:], left[0])
            at += columns[1] - columns[0]


SMEM = pl.BlockSpec(memory_space=pltpu.SMEM)
VMEM = pl.BlockSpec(memory_space=pltpu.VMEM)


def call(kernel, scalars, arrays, outs, scratch=()):
    return pl.pallas_call(
        kernel,
        out_shape=tuple(jax.ShapeDtypeStruct(shape, kind) for shape, kind in outs),
        in_specs=[SMEM] * len(scalars) + [VMEM] * len(arrays),
        out_specs=tuple([VMEM] * len(outs)),
        scratch_shapes=[pltpu.VMEM(shape, kind) for shape, kind in scratch],
    )(*scalars, *arrays)


def per_device(
    chain,
    docs,
    segments,
    lengths,
    query_weight,
    key_weight,
    value_weight,
    out_weight,
    norm_gain,
    gate_vector,
    gate_bias,
    memory_init,
    cotangent,
):
    segment, cot = segments[0, 0], cotangent[0, 0]
    count, width = segment.shape
    slots = memory_init.shape[0]
    kv2 = 2 * key_weight.shape[1]
    count_half = chain // 2
    own = slots // count_half
    devices = chain * docs
    place = lax.axis_index("chain")
    me = (place * docs + lax.axis_index("dp")).reshape(1, 1)
    mine = place % count_half
    gain, vector = norm_gain[None, :], gate_vector[None, :]
    bias = lax.dynamic_slice(gate_bias, (mine * own,), (own,))[:, None]
    mem_own = lax.dynamic_slice(memory_init, (mine * own, 0), (own, width)).astype(F32)

    bits = devices.bit_length() - 1
    low = docs.bit_length() - 1
    others = list(range(low + 1, bits))
    within = list(range(low))
    order_a = within + others
    order_b = others[:1] + within + others[1:]
    meet = low + 1
    cut = width // 2
    height = width // devices

    def table_of(order):
        table = []
        for b in range(devices // 2):
            table.append(sum(((b >> (bits - 2 - k)) & 1) << pos for k, pos in enumerate(order)))
        return tuple(table)

    def products(arrays, groups):
        outs, plan, ranges = [], [], {}
        for order, items in groups:
            lanes = sum(columns[1] - columns[0] for _, _, columns in items)
            outs += [((width // 4, lanes), F32)] * 2
            for lefts, _, _ in items:
                ranges.update({left: left[2] - left[1] for left in lefts if left[0] != "line"})
            plan.append((table_of(order), items))
        tall = max(LANES, sum(ranges.values()))
        return call(
            functools.partial(product_kernel, plan={"ins": len(arrays), "groups": plan}),
            [me],
            arrays,
            outs,
            [((devices, height, tall), F32), ((width // 2, tall), F32)],
        )

    def line(arrays, ranges):
        tall = sum(last - first for _, first, last in ranges)
        return call(
            functools.partial(line_kernel, table=table_of(order_a), ranges=ranges),
            [me],
            arrays,
            [((width // 2, tall), BF16)],
            [((devices, height, tall), F32)],
        )[0]

    def swap(rows, pos):
        return lax.ppermute(rows, ("chain", "dp"), [(i, i ^ (1 << pos)) for i in range(devices)])

    def fold(kept, got):
        half = kept.shape[0] // 2
        return kept[:half] + got[:half], kept[half:] + got[half:]

    def halved(kept, sent, order):
        for pos in order[:-1]:
            kept, sent = fold(kept, swap(sent, pos))
        return kept, swap(sent, order[-1])

    def joined(pairs):
        halves = [fold(*pair) for pair in pairs]
        return tuple(jnp.concatenate([half[i] for half in halves], axis=1) for i in (0, 1))

    halves = [list(range(count_half)), list(range(count_half, chain))]

    def trade(blocks):
        return lax.all_to_all(
            blocks, "chain", 0, 0, axis_index_groups=halves, tiled=True
        )

    def handed(rows, back):
        pairs = [(c, c + count_half) for c in range(count_half)]
        return lax.ppermute(rows, "chain", [(b, a) if back else (a, b) for a, b in pairs])

    q, kv, sn, s, c, u, pack0 = call(
        prepare_kernel,
        [lengths],
        [
            segment, cot, query_weight, key_weight, value_weight, out_weight, gain, vector,
            memory_init,
        ],
        [
            ((count, width), BF16),
            ((count, kv2), BF16),
            ((slots, width), BF16),
            ((slots, width), BF16),
            ((slots, width), F32),
            ((1, width), F32),
            ((2 * count, width), F32),
        ],
    )
    c_all = trade(c)
    pack0_far = swap(pack0, low)
    p_here, ret, end = call(
        functools.partial(owner_scan_kernel, count=count_half),
        [],
        [c_all, bias, u],
        [
            ((slots, width), F32),
            ((2, slots, LANES), F32),
            ((own, width + LANES), F32),
        ],
    )
    entering = handed(end, False)
    pack1, mem, stat, mkv = call(
        functools.partial(owner_kernel, count=count_half),
        [],
        [p_here, ret, entering, mem_own, out_weight, key_weight, value_weight, gain],
        [
            ((2 * slots, width), F32),
            ((slots, width), F32),
            ((2, slots, LANES), F32),
            ((slots, kv2), F32),
        ],
    )
    mkv_here = trade(mkv)
    pack1_far = swap(pack1, low)
    out, cr, dq, dkv_r, dmkv = call(
        read_kernel,
        [lengths],
        [segment, cot, q, kv, mkv_here, out_weight],
        [
            ((count, width), BF16),
            ((count, width), F32),
            ((count, width), F32),
            ((count, kv2), F32),
            ((slots, kv2), F32),
        ],
        [((count, width), BF16), ((count, width), BF16)],
    )
    dq_far = swap(dq, low)
    cr_far = swap(cr, low)
    dmkv_all = trade(dmkv)

    def rows_of(i, first, size):
        return (i, first, first + size)

    lined0 = line([pack0, pack0_far], [rows_of(0, 0, count), rows_of(1, 0, count)])
    lined1 = line(
        [pack1, pack1_far],
        [
            rows_of(0, 0, slots), rows_of(1, 0, slots),
            rows_of(0, slots, slots), rows_of(1, slots, slots),
        ],
    )
    early_items = (
        (("line", 0, 0, 2 * count),),
        (rows_of(1, 0, count), rows_of(2, 0, count)),
    )

    def split(items, *more):
        lefts, rights = items
        return [
            (order_a, [(lefts, rights, (0, cut))]),
            (order_b, [(lefts, rights, (cut, width)), *more]),
        ]

    early_a, sent_a, early_b, sent_b = products([lined0, dq, dq_far], split(early_items))
    early_a = halved(early_a, sent_a, order_a[:meet])
    early_b = halved(early_b, sent_b, order_b[:meet])
    r, later, stat_b, end, g0, gain_g = call(
        functools.partial(back_scan_kernel, count=count_half),
        [mine.reshape(1, 1)],
        [dmkv_all, mem, ret, stat, mem_own, out_weight, key_weight, value_weight, gain],
        [
            ((slots, width), F32),
            ((slots, width), F32),
            ((2, slots, LANES), F32),
            ((own, width + LANES), F32),
            ((slots, width), F32),
            ((1, width), F32),
        ],
    )
    r_far = swap(r, low)
    entering = handed(end, True)
    dmkv_far = swap(dmkv_all, low)
    g0_far = swap(g0, low)
    out_lefts = (
        rows_of(0, 0, count), rows_of(1, 0, count), ("line", 2, 2 * slots, 4 * slots),
    )
    out_rights = (
        rows_of(3, count, count), rows_of(4, count, count), rows_of(5, 0, slots), rows_of(6, 0, slots),
    )
    out_a, sent_a, out_b, sent_b = products(
        [cr, cr_far, lined1, pack0, pack0_far, r, r_far, g0, g0_far],
        split(
            (out_lefts, out_rights),
            ((rows_of(7, 0, slots), rows_of(8, 0, slots)), (), (0, slots)),
        ),
    )
    out_a = halved(out_a, sent_a, order_a[:meet])
    out_b = halved(out_b, sent_b, order_b[:meet])
    early_kept, early_got = halved(*joined([early_a, early_b]), order_a[meet:])
    out_kept, out_got = halved(*joined([out_a, out_b]), order_a[meet:])
    dc, vec = call(
        functools.partial(back_kernel, count=count_half),
        [],
        [later, stat_b, entering, pack1, c_all, ret, stat, u, out_weight, gain_g],
        [((slots, width), F32), ((3, width), F32)],
    )
    dc_here = trade(dc)
    slot_bits = [low] + order_a[:meet]
    parts = 1 << len(slot_bits)
    flat = me[0, 0]
    key = sum(
        ((flat >> pos) & 1) << (len(slot_bits) - 1 - k) for k, pos in enumerate(slot_bits)
    ).reshape(1, 1)
    dkv, kept_s, sent_s = call(
        finish_kernel,
        [key, lengths],
        [segment, s, kv, dc_here, dq, dkv_r, query_weight, key_weight, value_weight, vec],
        [((count, kv2), F32)] + [((slots // 2 + 8, width), F32)] * 2,
        [((parts, slots // parts, width), F32), ((count, kv2), BF16)],
    )
    got_s = swap(sent_s, low)
    dkv_far = swap(dkv, low)
    kv_left = (("line", 0, 0, 2 * count), ("line", 1, 0, 2 * slots))
    kv_right = (
        rows_of(2, 0, count), rows_of(3, 0, count), rows_of(4, 0, slots), rows_of(5, 0, slots),
    )
    late_a, sent_a, late_b, sent_b = products(
        [lined0, lined1, dkv, dkv_far, dmkv_all, dmkv_far],
        [
            (order_a, [(kv_left, kv_right, (0, kv2 // 2))]),
            (order_b, [(kv_left, kv_right, (kv2 // 2, kv2))]),
        ],
    )
    for pos in slot_bits[1:]:
        half = (kept_s.shape[0] - 8) // 2
        shared = kept_s[2 * half :] + got_s[2 * half :]
        sent_s = jnp.concatenate([kept_s[half : 2 * half] + got_s[half : 2 * half], shared], axis=0)
        kept_s = jnp.concatenate([kept_s[:half] + got_s[:half], shared], axis=0)
        got_s = swap(sent_s, pos)
    total = kept_s + got_s
    for pos in order_a[meet:]:
        total = total + swap(total, pos)
    slot_rows = total[:-8]
    for pos in reversed(slot_bits):
        slot_far = swap(slot_rows, pos)
        if pos != low:
            slot_rows = jnp.concatenate([slot_rows, slot_far], axis=0)
    late_a = halved(late_a, sent_a, order_a[:meet])
    late_b = halved(late_b, sent_b, order_b[:meet])
    late, got = halved(*joined([late_a, late_b]), order_a[meet:])
    g_kv = late + got
    g_query, g_out, g_small, g_mem = call(
        last_kernel,
        [key, me],
        [
            slot_rows, slot_far, total, sn, query_weight, memory_init, gain, vector,
            early_kept, early_got, out_kept, out_got,
        ],
        [((height, width), F32), ((height, width), F32), ((16, height), F32), ((slots, height), F32)],
        [((parts, slots // parts, width), F32), ((devices, height, 2 * slots), F32)],
    )
    return (
        out[None, None],
        g_query,
        g_kv[:, : kv2 // 2],
        g_kv[:, kv2 // 2 :],
        g_out,
        g_small[8],
        g_small[2],
        g_mem,
    )


def solution(mesh):
    in_specs = (
        P("dp", "chain", None, None),
        P("dp", "chain"),
        P(),
        P(),
        P(),
        P(),
        P(),
        P(),
        P(),
        P(),
        P("dp", "chain", None, None),
    )
    out_specs = (
        P("dp", "chain", None, None),
        P(("chain", "dp"), None),
        P(("chain", "dp"), None),
        P(("chain", "dp"), None),
        P(("chain", "dp"), None),
        P(("chain", "dp")),
        P(("chain", "dp")),
        P(None, ("chain", "dp")),
    )

    def step(*args):
        return per_device(mesh.shape["chain"], mesh.shape["dp"], *args)

    return jax.shard_map(
        step, mesh=mesh, in_specs=in_specs, out_specs=out_specs, check_vma=False
    )
```

```python
import functools

import jax
import jax.numpy as jnp
from jax import lax
from jax.experimental import pallas as pl
from jax.experimental.pallas import tpu as pltpu
from jax.sharding import PartitionSpec as P


HEAD = 64
LANES = 128
epsilon = 1e-05
score_scale = 0.125
F32 = jnp.float32
BF16 = jnp.bfloat16


def mm(a, b):
    return lax.dot_general(a, b, (((1,), (0,)), ((), ())), preferred_element_type=F32)


def mm_nt(a, b):
    return lax.dot_general(a, b, (((1,), (1,)), ((), ())), preferred_element_type=F32)


def inverse_rms(rows):
    return lax.rsqrt(jnp.mean(rows * rows, axis=-1, keepdims=True) + epsilon)


def low_lanes(shape):
    return lax.broadcasted_iota(jnp.int32, shape, 1) < HEAD


def padded(tile, odd):
    wide = tile.astype(F32)
    mine = low_lanes(wide.shape) != bool(odd)
    here = jnp.where(mine, wide, 0.0)
    there = pltpu.roll(here, HEAD, 1)
    low, high = (there, here) if odd else (here, there)
    return jnp.concatenate([low, high], axis=0).astype(BF16)


def unpadded(total, odd):
    rows = total.shape[0] // 2
    low_mask = low_lanes((rows, LANES))
    low = jnp.where(low_mask, total[:rows], 0.0)
    high = jnp.where(low_mask, 0.0, total[rows:])
    return high + pltpu.roll(low, HEAD, 1) if odd else low + pltpu.roll(high, HEAD, 1)


def softmax_rows(scores, allowed):
    width = scores.shape[0] // 2
    halves = []
    for part in (scores[:width], scores[width:]):
        part = jnp.where(allowed, part, -1e30)
        raised = jnp.exp(part - jnp.max(part, axis=0, keepdims=True))
        halves.append(raised / jnp.sum(raised, axis=0, keepdims=True))
    return jnp.concatenate(halves, axis=0)


def softmax_back(weights, d_weights):
    width = weights.shape[0] // 2
    halves = []
    for at in (0, width):
        w, d = weights[at : at + width], d_weights[at : at + width]
        halves.append(w * (d - jnp.sum(w * d, axis=0, keepdims=True)))
    return jnp.concatenate(halves, axis=0)


def split3(value):
    high = value.astype(BF16)
    rest = value - high.astype(F32)
    mid = rest.astype(BF16)
    return high, mid, (rest - mid.astype(F32)).astype(BF16)


def row_times(row, matrix, transposed):
    pieces = split3(row)
    stacked = jnp.concatenate(list(pieces) + [jnp.zeros_like(pieces[0])] * 13, axis=0)
    return jnp.sum((mm_nt if transposed else mm)(stacked, matrix), axis=0, keepdims=True)


def prepare_kernel(
    length, seg, wq, wk, wv, gain, mem0, q_o, kv_o, sn_o, s_o, c_o
):
    count = seg.shape[0]
    kv_width = wk.shape[1]
    rows = seg[...].astype(F32)
    start = mem0[...].astype(F32)
    g = gain[...]
    xn = (rows * inverse_rms(rows) * g).astype(BF16)
    sn = (start * inverse_rms(start) * g).astype(BF16)
    sn_o[...] = sn
    both = mm(jnp.concatenate([xn, sn], axis=0), wq[...]) * score_scale
    q_o[...] = both[:count].astype(BF16)
    s_o[...] = both[count:].astype(BF16)
    kv_o[:, :kv_width] = mm(xn, wk[...]).astype(BF16)
    kv_o[:, kv_width:] = mm(xn, wv[...]).astype(BF16)
    slots = mem0.shape[0]
    allowed = lax.broadcasted_iota(jnp.int32, (count, slots), 0) < length[0, 0]
    pairs = s_o.shape[1] // LANES
    groups = kv_width // HEAD
    for group in range(groups):
        at, odd = (group // 2) * LANES, group % 2
        keys = padded(kv_o[:, at : at + LANES], odd)
        values_t = padded(kv_o[:, kv_width + at : kv_width + at + LANES], odd).T
        for pair in range(group * pairs // groups, (group + 1) * pairs // groups):
            lanes = slice(pair * LANES, (pair + 1) * LANES)
            weights = softmax_rows(mm_nt(keys, s_o[:, lanes]), allowed).astype(BF16)
            c_o[:, lanes] = mm(values_t, weights).T.astype(BF16).astype(F32)


def rows_kernel(length, seg, cot, wo, gain, vector, both_o, u_o):
    count = seg.shape[0]
    rows = seg[...].astype(F32)
    both_o[:count] = (rows * inverse_rms(rows) * gain[...]).astype(BF16).astype(F32)
    valid = lax.broadcasted_iota(jnp.int32, (count, 1), 0) < length[0, 0]
    both_o[count:] = jnp.where(valid, cot[...].astype(F32), 0.0)
    u_o[...] = row_times(vector[...], wo[...], True)


def tiled(rows, times):
    return jnp.concatenate([rows] * times, axis=0)


def owner_scan_kernel(call, bias, u, p_o, stat_o, end_o, *, count):
    rows, width = call.shape
    own = rows // count
    logits = jnp.sum(call[...] * u[...], axis=1, keepdims=True) + tiled(bias[...], count)
    stat_o[0] = jnp.broadcast_to(jax.nn.sigmoid(logits), (rows, LANES))
    memory = jnp.zeros((own, width), F32)
    keep = jnp.ones((own, LANES), F32)
    for c in range(count):
        at = slice(c * own, (c + 1) * own)
        p_o[at, :] = memory
        stat_o[1, at, :] = keep
        ret = stat_o[0, at, :]
        memory = ret[:, :1] * memory + (1.0 - ret[:, :1]) * call[at, :]
        keep = keep * ret
    end_o[:, :width] = memory
    end_o[:, width:] = 1.0 - keep


def owner_kernel(
    p_in, stat, handed, mem_own, wo, wk, wv, gain, both_o, mem_o, stat_o, mkv_o, *, count
):
    rows, width = p_in.shape
    keep_here = stat[1]
    p = p_in[...] + keep_here[:, :1] * tiled(handed[:, :width], count)
    keep = keep_here * tiled(1.0 - handed[:, width:], count)
    both_o[rows:] = p
    mem = keep[:, :1] * tiled(mem_own[...], count) + mm(p.astype(BF16), wo[...])
    mem_o[...] = mem
    inverse = inverse_rms(mem)
    stat_o[0] = keep
    stat_o[1] = jnp.broadcast_to(inverse, (rows, LANES))
    mn = (mem * inverse * gain[...]).astype(BF16)
    both_o[:rows] = mn.astype(F32)
    kv_width = wk.shape[1]
    mkv_o[:, :kv_width] = mm(mn, wk[...]).astype(BF16).astype(F32)
    mkv_o[:, kv_width:] = mm(mn, wv[...]).astype(BF16).astype(F32)


def read_kernel(
    length, seg, cot, q, kv, mkv, wo, out_o, cr_o, dq_o, dkv_o, dmkv_o, dcr_s, cr_s
):
    count, width = q.shape
    slots = mkv.shape[0]
    kv_width = kv.shape[1] // 2
    pairs = width // LANES
    groups = kv_width // HEAD
    valid = lax.broadcasted_iota(jnp.int32, (count, 1), 0) < length[0, 0]
    d_out = jnp.where(valid, cot[...].astype(F32), 0.0).astype(BF16)
    dcr_s[...] = mm_nt(d_out, wo[...]).astype(BF16)
    key_at = lax.broadcasted_iota(jnp.int32, (slots + count, count), 0) - slots
    query_at = lax.broadcasted_iota(jnp.int32, (slots + count, count), 1)
    allowed = (key_at < 0) | ((key_at <= query_at) & (key_at < length[0, 0]))
    d_keys = [None] * groups
    d_values = [None] * groups
    for group in range(groups):
        at, odd = (group // 2) * LANES, group % 2
        keys = padded(
            jnp.concatenate(
                [mkv[:, at : at + LANES], kv[:, at : at + LANES].astype(F32)], axis=0
            ),
            odd,
        )
        at_v = kv_width + at
        values = padded(
            jnp.concatenate(
                [mkv[:, at_v : at_v + LANES], kv[:, at_v : at_v + LANES].astype(F32)], axis=0
            ),
            odd,
        )
        keys_t, values_t = keys.T, values.T
        dk = dv = None
        for pair in range(group * pairs // groups, (group + 1) * pairs // groups):
            lanes = slice(pair * LANES, (pair + 1) * LANES)
            q_tile = q[:, lanes]
            weights = softmax_rows(mm_nt(keys, q_tile), allowed)
            rounded = weights.astype(BF16)
            context = mm(values_t, rounded).T.astype(BF16)
            cr_s[:, lanes] = context
            cr_o[:, lanes] = context.astype(F32)
            d_tile = dcr_s[:, lanes]
            d_weights = mm_nt(values, d_tile).astype(BF16).astype(F32)
            d_scores = softmax_back(weights, d_weights).astype(BF16)
            dq = mm(keys_t, d_scores).T.astype(BF16).astype(F32)
            dq_o[:, lanes] = dq * score_scale
            dk_here = mm(d_scores, q_tile)
            dv_here = mm(rounded, d_tile)
            dk = dk_here if dk is None else dk + dk_here
            dv = dv_here if dv is None else dv + dv_here
        d_keys[group] = unpadded(dk, odd)
        d_values[group] = unpadded(dv, odd)
    for side, parts in ((0, d_keys), (kv_width, d_values)):
        for tile in range(groups // 2):
            lanes = slice(side + tile * LANES, side + (tile + 1) * LANES)
            total = (parts[2 * tile] + parts[2 * tile + 1]).astype(BF16).astype(F32)
            dmkv_o[:, lanes] = total[:slots]
            dkv_o[:, lanes] = total[slots:]
    out_o[...] = (seg[...].astype(F32) + mm(cr_s[...], wo[...])).astype(BF16)


def back_scan_kernel(
    place, dmkv, mem, ret, stat, mem_own, wo, wk, wv, gain,
    r_o, later_o, stat_o, end_o, g0_o, gain_o, *, count,
):
    rows, width = mem.shape
    own = rows // count
    kv_width = wk.shape[1]
    dmb = dmkv[...].astype(BF16)
    dmn = mm_nt(dmb[:, :kv_width], wk[...]) + mm_nt(dmb[:, kv_width:], wv[...])
    inverse = stat[1][:, :1]
    keep = stat[0][:, :1]
    memory = mem[...]
    gain_o[...] = jnp.sum(dmn * memory * inverse, axis=0, keepdims=True)
    scaled = dmn * gain[...]
    inner = jnp.sum(scaled * memory, axis=1, keepdims=True) * (1.0 / width)
    r = inverse * scaled - memory * (inverse * inverse * inverse * inner)
    rounded = r.astype(BF16)
    r_o[...] = rounded.astype(F32)
    q = jnp.sum(r * tiled(mem_own[...], count), axis=1, keepdims=True)
    kept = keep * r
    g0 = kept[:own]
    for c in range(1, count):
        g0 = g0 + kept[c * own : (c + 1) * own]
    at = lax.broadcasted_iota(jnp.int32, (rows, 1), 0)
    first = place[0, 0] * own
    g0_o[...] = jnp.where((at >= first) & (at < first + own), tiled(g0, count), 0.0)
    turned = mm_nt(rounded, wo[...])
    q = jnp.broadcast_to(q, (rows, LANES))
    later = jnp.zeros((own, width), F32)
    later_q = jnp.zeros((own, LANES), F32)
    passed = jnp.ones((own, LANES), F32)
    for c in reversed(range(count)):
        at = slice(c * own, (c + 1) * own)
        retain = ret[0, at, :]
        later_o[at, :] = later
        stat_o[0, at, :] = later_q
        stat_o[1, at, :] = passed
        later = turned[at] + retain[:, :1] * later
        later_q = q[at] + retain * later_q
        passed = passed * retain
    end_o[:, :width] = later
    end_o[:, width:] = later_q


def back_kernel(later, stat_b, handed, both, call, ret, stat, u, wo, gain_g, dc_o, vec_o, *, count):
    rows, width = later.shape
    passed = stat_b[1][:, :1]
    ahead = later[...] + passed * tiled(handed[:, :width], count)
    ahead_q = stat_b[0][:, :1] + passed * tiled(handed[:, width : width + 1], count)
    context = call[...]
    retain = ret[0][:, :1]
    d_retain = stat[0][:, :1] * ahead_q + jnp.sum(
        ahead * (both[rows:] - context), axis=1, keepdims=True
    )
    dz = d_retain * retain * (1.0 - retain)
    dc_o[...] = (1.0 - retain) * ahead + dz * u[...]
    v = jnp.sum(dz * context, axis=0, keepdims=True)
    vec_o[0:1, :] = gain_g[...]
    vec_o[1:2, :] = v
    vec_o[2:3, :] = row_times(v, wo[...], False)


def finish_kernel(
    key, length, seg, s, kv, dc, dq, dkv_r, wq, wk, wv, vec,
    dkv_o, keep_o, send_o, dqs_s, dkv_s,
):
    count, width = seg.shape
    slots = s.shape[0]
    pieces, piece, _ = dqs_s.shape
    kv_width = wk.shape[1]
    pairs = width // LANES
    groups = kv_width // HEAD
    allowed = lax.broadcasted_iota(jnp.int32, (count, slots), 0) < length[0, 0]
    d_keys = [None] * groups
    d_values = [None] * groups
    for group in range(groups):
        at, odd = (group // 2) * LANES, group % 2
        keys = padded(kv[:, at : at + LANES], odd)
        values = padded(kv[:, kv_width + at : kv_width + at + LANES], odd)
        keys_t = keys.T
        dk = dv = None
        for pair in range(group * pairs // groups, (group + 1) * pairs // groups):
            lanes = slice(pair * LANES, (pair + 1) * LANES)
            s_tile = s[:, lanes]
            weights = softmax_rows(mm_nt(keys, s_tile), allowed)
            d_tile = dc[:, lanes].astype(BF16)
            d_weights = mm_nt(values, d_tile).astype(BF16).astype(F32)
            d_scores = softmax_back(weights, d_weights).astype(BF16)
            dqs = mm(keys_t, d_scores).T.astype(BF16).astype(F32)
            dqs = dqs * score_scale
            for t in range(pieces):
                dqs_s[t, :, lanes] = dqs[t * piece : (t + 1) * piece]
            dk_here = mm(d_scores, s_tile)
            dv_here = mm(weights.astype(BF16), d_tile)
            dk = dk_here if dk is None else dk + dk_here
            dv = dv_here if dv is None else dv + dv_here
        d_keys[group] = unpadded(dk, odd)
        d_values[group] = unpadded(dv, odd)
    for side, parts in ((0, d_keys), (kv_width, d_values)):
        for tile in range(groups // 2):
            lanes = slice(side + tile * LANES, side + (tile + 1) * LANES)
            total = (parts[2 * tile] + parts[2 * tile + 1]).astype(BF16).astype(F32)
            total = (total + dkv_r[:, lanes]).astype(BF16)
            dkv_s[:, lanes] = total
            dkv_o[:, lanes] = total.astype(F32)
    dxn = mm_nt(dq[...].astype(BF16), wq[...])
    dxn = dxn + mm_nt(dkv_s[:, :kv_width], wk[...]) + mm_nt(dkv_s[:, kv_width:], wv[...])
    rows = seg[...].astype(F32)
    gain_here = jnp.sum(dxn * (rows * inverse_rms(rows)), axis=0, keepdims=True)
    step = piece + 8
    sums = jnp.concatenate(
        [vec[0:1, :] + gain_here, vec[1:3, :], jnp.zeros((5, width), F32)], axis=0
    )
    for t in range(pieces // 2):
        at = slice(t * step, t * step + piece)
        keep_o[at, :] = dqs_s[key[0, 0] ^ t]
        send_o[at, :] = dqs_s[key[0, 0] ^ (t + pieces // 2)]
        keep_o[t * step + piece : (t + 1) * step] = sums
        send_o[t * step + piece : (t + 1) * step] = sums


def last_kernel(
    key, me, near, far, sn, wq, mem0, gain, vector, kept, got, kept_out, got_out,
    query_o, out_o, gain_o, gate_o, mem_o, dqs_s, turn_s,
):
    slots, width = sn.shape
    pieces, piece, _ = dqs_s.shape
    height = kept.shape[0]
    for t in range(pieces // 2):
        at = slice(t * (piece + 8), t * (piece + 8) + piece)
        dqs_s[key[0, 0] ^ t] = near[at]
        dqs_s[key[0, 0] ^ (t + pieces // 2)] = far[at]
    d_slots = jnp.concatenate([dqs_s[t] for t in range(pieces)], axis=0).astype(BF16)
    turned = sn[...].astype(F32).T
    for b in range(width // height):
        turn_s[b, :, :slots] = turned[b * height : (b + 1) * height]
    rows = turn_s[me[0, 0], :, :slots].astype(BF16)
    query_o[...] = kept[...] + got[...] + mm(rows, d_slots)
    dsn = mm_nt(d_slots, wq[...])
    start = mem0[...].astype(F32)
    inverse = inverse_rms(start)
    gain_row = jnp.sum(dsn * (start * inverse), axis=0, keepdims=True)
    scaled = dsn * gain[...]
    inner = jnp.sum(scaled * start, axis=1, keepdims=True) * (1.0 / width)
    d_start = inverse * scaled - start * (inverse * inverse * inverse * inner)
    sums = near[piece : piece + 8]
    small = jnp.concatenate(
        [sums, sums[0:1] + gain_row, jnp.zeros((slots - 9, width), F32)], axis=0
    )
    columns = jnp.concatenate([d_start, small], axis=0).T
    for b in range(width // height):
        turn_s[b] = columns[b * height : (b + 1) * height]
    mine = turn_s[me[0, 0]]
    held = kept_out[:, width:] + got_out[:, width:]
    mem_o[...] = mine[:, :slots] + held
    across = mine[:, slots:].T
    gain_o[...] = across[8:9]
    gate_o[...] = across[2:3]
    out_o[...] = (
        kept_out[:, :width]
        + got_out[:, :width]
        + mine[:, slots + 1 : slots + 2] * vector[...]
    )


def line_kernel(me, *refs, table, ranges):
    ins, out, turned = refs[:-2], refs[-2], refs[-1]
    blocks, height, _ = turned.shape
    lane = 0
    for i, first, last in ranges:
        across = slice(lane, lane + last - first)
        tall = ins[i][first:last].T
        for b in range(blocks):
            turned[b, :, across] = tall[b * height : (b + 1) * height]
        lane += last - first
    for b in range(blocks // 2):
        out[b * height : (b + 1) * height, :] = turned[me[0, 0] ^ table[b]].astype(BF16)


def product_kernel(me, *refs, plan):
    ins = refs[: plan["ins"]]
    outs = list(refs[plan["ins"] : -2])
    turned, lined = refs[-2:]
    blocks, height, _ = turned.shape
    kind = turned.dtype
    places, lane = {}, 0
    for _, _, items in plan["groups"]:
        for lefts, _, _ in items:
            for left in lefts:
                if left in places:
                    continue
                if left[0] == "line":
                    places[left] = (ins[left[1]], slice(left[2], left[3]))
                    continue
                i, first, last = left
                rows = ins[i][first:last].astype(kind)
                across = slice(lane, lane + last - first)
                places[left] = (lined, across)
                tall = rows.T
                for b in range(blocks):
                    turned[b, :, across] = tall[b * height : (b + 1) * height]
                lane += last - first
    base = plan["groups"][0][0]
    for b in range(blocks // 2 if lane else 0):
        lined[b * height : (b + 1) * height, :lane] = turned[me[0, 0] ^ base[b], :, :lane]
    where = {dest: b for b, dest in enumerate(base)}
    for table, pieces, items in plan["groups"]:
        size = blocks // 2 // pieces
        runs = []
        for dest in table:
            b = where[dest]
            if runs and runs[-1][1] == b:
                runs[-1][1] = b + 1
            else:
                runs.append([b, b + 1])
        offset = 0
        cuts = []
        for lo, hi in runs:
            while lo < hi:
                take = min(hi - lo, size - offset % size)
                cuts.append((offset, lo, lo + take))
                offset += take
                lo += take
        at = 0
        for lefts, rights, columns in items:
            if rights:
                right = jnp.concatenate(
                    [
                        ins[i][first:last, columns[0] : columns[1]].astype(BF16)
                        for i, first, last in rights
                    ],
                    axis=0,
                )
            for offset, lo, hi in cuts:
                out = outs[offset // size]
                first = offset % size * height
                to = slice(first, first + (hi - lo) * height)
                left = [
                    places[part][0][lo * height : hi * height, places[part][1]] for part in lefts
                ]
                if rights:
                    left = jnp.concatenate([part.astype(BF16) for part in left], axis=1)
                    out[to, at : at + right.shape[1]] = mm(left, right)
                else:
                    out[to, at : at + left[0].shape[1]] = sum(left[1:], left[0])
            at += columns[1] - columns[0]
        outs = outs[pieces:]


SMEM = pl.BlockSpec(memory_space=pltpu.SMEM)
VMEM = pl.BlockSpec(memory_space=pltpu.VMEM)


def call(kernel, scalars, arrays, outs, scratch=()):
    return pl.pallas_call(
        kernel,
        out_shape=tuple(jax.ShapeDtypeStruct(shape, kind) for shape, kind in outs),
        in_specs=[SMEM] * len(scalars) + [VMEM] * len(arrays),
        out_specs=tuple([VMEM] * len(outs)),
        scratch_shapes=[pltpu.VMEM(shape, kind) for shape, kind in scratch],
    )(*scalars, *arrays)


def per_device(
    chain,
    docs,
    segments,
    lengths,
    query_weight,
    key_weight,
    value_weight,
    out_weight,
    norm_gain,
    gate_vector,
    gate_bias,
    memory_init,
    cotangent,
):
    segment, cot = segments[0, 0], cotangent[0, 0]
    count, width = segment.shape
    slots = memory_init.shape[0]
    kv2 = 2 * key_weight.shape[1]
    count_half = chain // 2
    own = slots // count_half
    devices = chain * docs
    place = lax.axis_index("chain")
    me = (place * docs + lax.axis_index("dp")).reshape(1, 1)
    mine = place % count_half
    gain, vector = norm_gain[None, :], gate_vector[None, :]
    bias = lax.dynamic_slice(gate_bias, (mine * own,), (own,))[:, None]
    mem_own = lax.dynamic_slice(memory_init, (mine * own, 0), (own, width)).astype(F32)

    bits = devices.bit_length() - 1
    low = docs.bit_length() - 1
    others = list(range(low + 1, bits))
    within = list(range(low))
    order_a = within + others
    order_b = others[:1] + within + others[1:]
    meet = low + 1
    cut = width // 2
    height = width // devices

    def table_of(order):
        table = []
        for b in range(devices // 2):
            table.append(sum(((b >> (bits - 2 - k)) & 1) << pos for k, pos in enumerate(order)))
        return tuple(table)

    def products(arrays, groups):
        outs, plan, ranges = [], [], {}
        for order, pieces, items in groups:
            lanes = sum(columns[1] - columns[0] for _, _, columns in items)
            outs += [((width // 2 // pieces, lanes), F32)] * pieces
            for lefts, _, _ in items:
                ranges.update({left: left[2] - left[1] for left in lefts if left[0] != "line"})
            plan.append((table_of(order), pieces, items))
        tall = max(LANES, sum(ranges.values()))
        return call(
            functools.partial(product_kernel, plan={"ins": len(arrays), "groups": plan}),
            [me],
            arrays,
            outs,
            [((devices, height, tall), F32), ((width // 2, tall), F32)],
        )

    def line(arrays, ranges):
        tall = sum(last - first for _, first, last in ranges)
        return call(
            functools.partial(line_kernel, table=table_of(order_a), ranges=ranges),
            [me],
            arrays,
            [((width // 2, tall), BF16)],
            [((devices, height, tall), F32)],
        )[0]

    def swap(rows, pos):
        return lax.ppermute(rows, ("chain", "dp"), [(i, i ^ (1 << pos)) for i in range(devices)])

    spread = 1 << meet
    masks = [
        sum(((t >> (meet - 1 - k)) & 1) << pos for k, pos in enumerate(order_a[:meet]))
        for t in range(spread)
    ]

    def direct(sent):
        got = []
        for t, part in enumerate(sent):
            mask = masks[t + 1]
            got.append(
                lax.ppermute(
                    part, ("chain", "dp"), [(i, i ^ mask) for i in range(devices)]
                )
            )
        return got

    def split_sum(parts):
        half = parts[0].shape[0] // 2
        return sum(part[:half] for part in parts), sum(part[half:] for part in parts)

    def fold(kept, got):
        half = kept.shape[0] // 2
        return kept[:half] + got[:half], kept[half:] + got[half:]

    def halved(kept, sent, order):
        for pos in order[:-1]:
            kept, sent = fold(kept, swap(sent, pos))
        return kept, swap(sent, order[-1])

    def joined(pairs):
        halves = [fold(*pair) for pair in pairs]
        return tuple(jnp.concatenate([half[i] for half in halves], axis=1) for i in (0, 1))

    halves = [list(range(count_half)), list(range(count_half, chain))]

    def trade(blocks):
        return lax.all_to_all(
            blocks, "chain", 0, 0, axis_index_groups=halves, tiled=True
        )

    def handed(rows, back):
        pairs = [(c, c + count_half) for c in range(count_half)]
        return lax.ppermute(rows, "chain", [(b, a) if back else (a, b) for a, b in pairs])

    q, kv, sn, s, c = call(
        prepare_kernel,
        [lengths],
        [segment, query_weight, key_weight, value_weight, gain, memory_init],
        [
            ((count, width), BF16),
            ((count, kv2), BF16),
            ((slots, width), BF16),
            ((slots, width), BF16),
            ((slots, width), F32),
        ],
    )
    c_all = trade(c)
    pack0, u = call(
        rows_kernel,
        [lengths],
        [segment, cot, out_weight, gain, vector],
        [((2 * count, width), F32), ((1, width), F32)],
    )
    pack0_far = swap(pack0, low)
    p_here, ret, end = call(
        functools.partial(owner_scan_kernel, count=count_half),
        [],
        [c_all, bias, u],
        [
            ((slots, width), F32),
            ((2, slots, LANES), F32),
            ((own, width + LANES), F32),
        ],
    )
    entering = handed(end, False)
    pack1, mem, stat, mkv = call(
        functools.partial(owner_kernel, count=count_half),
        [],
        [p_here, ret, entering, mem_own, out_weight, key_weight, value_weight, gain],
        [
            ((2 * slots, width), F32),
            ((slots, width), F32),
            ((2, slots, LANES), F32),
            ((slots, kv2), F32),
        ],
    )
    mkv_here = trade(mkv)
    pack1_far = swap(pack1, low)
    out, cr, dq, dkv_r, dmkv = call(
        read_kernel,
        [lengths],
        [segment, cot, q, kv, mkv_here, out_weight],
        [
            ((count, width), BF16),
            ((count, width), F32),
            ((count, width), F32),
            ((count, kv2), F32),
            ((slots, kv2), F32),
        ],
        [((count, width), BF16), ((count, width), BF16)],
    )
    dq_far = swap(dq, low)
    cr_far = swap(cr, low)
    dmkv_all = trade(dmkv)

    def rows_of(i, first, size):
        return (i, first, first + size)

    lined0 = line([pack0, pack0_far], [rows_of(0, 0, count), rows_of(1, 0, count)])
    lined1 = line(
        [pack1, pack1_far],
        [
            rows_of(0, 0, slots), rows_of(1, 0, slots),
            rows_of(0, slots, slots), rows_of(1, slots, slots),
        ],
    )
    early_items = (
        (("line", 0, 0, 2 * count),),
        (rows_of(1, 0, count), rows_of(2, 0, count)),
    )

    def split(items, *more):
        lefts, rights = items
        return [
            (order_a, 2, [(lefts, rights, (0, cut))]),
            (order_b, 2, [(lefts, rights, (cut, width)), *more]),
        ]

    early, *sent = products([lined0, dq, dq_far], [(order_a, spread, [(*early_items, (0, width))])])
    early_far = direct(sent)
    early = split_sum([early, *early_far])
    r, later, stat_b, end, g0, gain_g = call(
        functools.partial(back_scan_kernel, count=count_half),
        [mine.reshape(1, 1)],
        [dmkv_all, mem, ret, stat, mem_own, out_weight, key_weight, value_weight, gain],
        [
            ((slots, width), F32),
            ((slots, width), F32),
            ((2, slots, LANES), F32),
            ((own, width + LANES), F32),
            ((slots, width), F32),
            ((1, width), F32),
        ],
    )
    r_far = swap(r, low)
    entering = handed(end, True)
    dmkv_far = swap(dmkv_all, low)
    g0_far = swap(g0, low)
    out_lefts = (
        rows_of(0, 0, count), rows_of(1, 0, count), ("line", 2, 2 * slots, 4 * slots),
    )
    out_rights = (
        rows_of(3, count, count), rows_of(4, count, count), rows_of(5, 0, slots), rows_of(6, 0, slots),
    )
    out_a, sent_a, out_b, sent_b = products(
        [cr, cr_far, lined1, pack0, pack0_far, r, r_far, g0, g0_far],
        split(
            (out_lefts, out_rights),
            ((rows_of(7, 0, slots), rows_of(8, 0, slots)), (), (0, slots)),
        ),
    )
    out_a = halved(out_a, sent_a, order_a[:meet])
    out_b = halved(out_b, sent_b, order_b[:meet])
    early_kept, early_got = halved(*early, order_a[meet:])
    out_kept, out_got = halved(*joined([out_a, out_b]), order_a[meet:])
    dc, vec = call(
        functools.partial(back_kernel, count=count_half),
        [],
        [later, stat_b, entering, pack1, c_all, ret, stat, u, out_weight, gain_g],
        [((slots, width), F32), ((3, width), F32)],
    )
    dc_here = trade(dc)
    slot_bits = [low] + order_a[:meet]
    parts = 1 << len(slot_bits)
    flat = me[0, 0]
    key = sum(
        ((flat >> pos) & 1) << (len(slot_bits) - 1 - k) for k, pos in enumerate(slot_bits)
    ).reshape(1, 1)
    step = slots // parts + 8
    dkv, kept_s, sent_s = call(
        finish_kernel,
        [key, lengths],
        [segment, s, kv, dc_here, dq, dkv_r, query_weight, key_weight, value_weight, vec],
        [((count, kv2), F32)] + [((spread * step, width), F32)] * 2,
        [((parts, slots // parts, width), F32), ((count, kv2), BF16)],
    )
    got_s = swap(sent_s, low)
    dkv_far = swap(dkv, low)
    kv_left = (("line", 0, 0, 2 * count), ("line", 1, 0, 2 * slots))
    kv_right = (
        rows_of(2, 0, count), rows_of(3, 0, count), rows_of(4, 0, slots), rows_of(5, 0, slots),
    )
    late, *sent = products(
        [lined0, lined1, dkv, dkv_far, dmkv_all, dmkv_far],
        [(order_a, spread, [(kv_left, kv_right, (0, kv2))])],
    )
    mine_s, *sent_s = [
        kept_s[t * step : (t + 1) * step] + got_s[t * step : (t + 1) * step]
        for t in range(spread)
    ]
    total = sum(direct(sent_s), mine_s)
    for pos in order_a[meet:]:
        total = total + swap(total, pos)
    near = jnp.concatenate([total, *direct([total] * (spread - 1))], axis=0)
    far = swap(near, low)
    late, got = halved(*split_sum([late, *direct(sent)]), order_a[meet:])
    g_kv = late + got
    g_query, g_out, g_gain, g_gate, g_mem = call(
        last_kernel,
        [key, me],
        [
            near, far, sn, query_weight, memory_init, gain, vector,
            early_kept, early_got, out_kept, out_got,
        ],
        [((height, width), F32)] * 2 + [((1, height), F32)] * 2 + [((height, slots), F32)],
        [((parts, slots // parts, width), F32), ((devices, height, 2 * slots), F32)],
    )
    return (
        out[None, None],
        g_query,
        g_kv[:, : kv2 // 2],
        g_kv[:, kv2 // 2 :],
        g_out,
        g_gain[0],
        g_gate[0],
        g_mem.T,
    )


def solution(mesh):
    in_specs = (
        P("dp", "chain", None, None),
        P("dp", "chain"),
        P(),
        P(),
        P(),
        P(),
        P(),
        P(),
        P(),
        P(),
        P("dp", "chain", None, None),
    )
    out_specs = (
        P("dp", "chain", None, None),
        P(("chain", "dp"), None),
        P(("chain", "dp"), None),
        P(("chain", "dp"), None),
        P(("chain", "dp"), None),
        P(("chain", "dp")),
        P(("chain", "dp")),
        P(None, ("chain", "dp")),
    )

    def step(*args):
        return per_device(mesh.shape["chain"], mesh.shape["dp"], *args)

    return jax.shard_map(
        step, mesh=mesh, in_specs=in_specs, out_specs=out_specs, check_vma=False
    )
```

```python
import functools

import jax
import jax.numpy as jnp
from jax import lax
from jax.experimental import pallas as pl
from jax.experimental.pallas import tpu as pltpu
from jax.sharding import PartitionSpec as P


HEAD = 64
LANES = 128
epsilon = 1e-05
score_scale = 0.125
F32 = jnp.float32
BF16 = jnp.bfloat16


def mm(a, b):
    return lax.dot_general(a, b, (((1,), (0,)), ((), ())), preferred_element_type=F32)


def mm_nt(a, b):
    return lax.dot_general(a, b, (((1,), (1,)), ((), ())), preferred_element_type=F32)


def inverse_rms(rows):
    return lax.rsqrt(jnp.mean(rows * rows, axis=-1, keepdims=True) + epsilon)


def low_lanes(shape):
    return lax.broadcasted_iota(jnp.int32, shape, 1) < HEAD


def padded(tile, odd):
    wide = tile.astype(F32)
    mine = low_lanes(wide.shape) != bool(odd)
    here = jnp.where(mine, wide, 0.0)
    there = pltpu.roll(here, HEAD, 1)
    low, high = (there, here) if odd else (here, there)
    return jnp.concatenate([low, high], axis=0).astype(BF16)


def unpadded(total, odd):
    rows = total.shape[0] // 2
    low_mask = low_lanes((rows, LANES))
    low = jnp.where(low_mask, total[:rows], 0.0)
    high = jnp.where(low_mask, 0.0, total[rows:])
    return high + pltpu.roll(low, HEAD, 1) if odd else low + pltpu.roll(high, HEAD, 1)


def softmax_rows(scores, allowed):
    width = scores.shape[0] // 2
    halves = []
    for part in (scores[:width], scores[width:]):
        part = jnp.where(allowed, part, -1e30)
        raised = jnp.exp(part - jnp.max(part, axis=0, keepdims=True))
        halves.append(raised / jnp.sum(raised, axis=0, keepdims=True))
    return jnp.concatenate(halves, axis=0)


def softmax_back(weights, d_weights):
    width = weights.shape[0] // 2
    halves = []
    for at in (0, width):
        w, d = weights[at : at + width], d_weights[at : at + width]
        halves.append(w * (d - jnp.sum(w * d, axis=0, keepdims=True)))
    return jnp.concatenate(halves, axis=0)


def split3(value):
    high = value.astype(BF16)
    rest = value - high.astype(F32)
    mid = rest.astype(BF16)
    return high, mid, (rest - mid.astype(F32)).astype(BF16)


def row_times(row, matrix, transposed):
    pieces = split3(row)
    stacked = jnp.concatenate(list(pieces) + [jnp.zeros_like(pieces[0])] * 13, axis=0)
    return jnp.sum((mm_nt if transposed else mm)(stacked, matrix), axis=0, keepdims=True)


def prepare_kernel(
    length, seg, wq, wk, wv, gain, mem0, q_o, kv_o, sn_o, s_o, c_o
):
    count = seg.shape[0]
    kv_width = wk.shape[1]
    rows = seg[...].astype(F32)
    start = mem0[...].astype(F32)
    g = gain[...]
    xn = (rows * inverse_rms(rows) * g).astype(BF16)
    sn = (start * inverse_rms(start) * g).astype(BF16)
    sn_o[...] = sn
    both = mm(jnp.concatenate([xn, sn], axis=0), wq[...]) * score_scale
    q_o[...] = both[:count].astype(BF16)
    s_o[...] = both[count:].astype(BF16)
    kv_o[:, :kv_width] = mm(xn, wk[...]).astype(BF16)
    kv_o[:, kv_width:] = mm(xn, wv[...]).astype(BF16)
    slots = mem0.shape[0]
    allowed = lax.broadcasted_iota(jnp.int32, (count, slots), 0) < length[0, 0]
    pairs = s_o.shape[1] // LANES
    groups = kv_width // HEAD
    for group in range(groups):
        at, odd = (group // 2) * LANES, group % 2
        keys = padded(kv_o[:, at : at + LANES], odd)
        values_t = padded(kv_o[:, kv_width + at : kv_width + at + LANES], odd).T
        for pair in range(group * pairs // groups, (group + 1) * pairs // groups):
            lanes = slice(pair * LANES, (pair + 1) * LANES)
            weights = softmax_rows(mm_nt(keys, s_o[:, lanes]), allowed).astype(BF16)
            c_o[:, lanes] = mm(values_t, weights).T.astype(BF16).astype(F32)


def rows_kernel(length, seg, cot, wo, gain, vector, both_o, u_o):
    count = seg.shape[0]
    rows = seg[...].astype(F32)
    both_o[:count] = (rows * inverse_rms(rows) * gain[...]).astype(BF16).astype(F32)
    valid = lax.broadcasted_iota(jnp.int32, (count, 1), 0) < length[0, 0]
    both_o[count:] = jnp.where(valid, cot[...].astype(F32), 0.0)
    u_o[...] = row_times(vector[...], wo[...], True)


def tiled(rows, times):
    return jnp.concatenate([rows] * times, axis=0)


def owner_scan_kernel(call, bias, u, p_o, stat_o, end_o, *, count):
    rows, width = call.shape
    own = rows // count
    logits = jnp.sum(call[...] * u[...], axis=1, keepdims=True) + tiled(bias[...], count)
    stat_o[0] = jnp.broadcast_to(jax.nn.sigmoid(logits), (rows, LANES))
    memory = jnp.zeros((own, width), F32)
    keep = jnp.ones((own, LANES), F32)
    for c in range(count):
        at = slice(c * own, (c + 1) * own)
        p_o[at, :] = memory
        stat_o[1, at, :] = keep
        ret = stat_o[0, at, :]
        memory = ret[:, :1] * memory + (1.0 - ret[:, :1]) * call[at, :]
        keep = keep * ret
    end_o[:, :width] = memory
    end_o[:, width:] = 1.0 - keep


def owner_kernel(
    p_in, stat, handed, mem_own, wo, wk, wv, gain, both_o, mem_o, stat_o, mkv_o, *, count
):
    rows, width = p_in.shape
    keep_here = stat[1]
    p = p_in[...] + keep_here[:, :1] * tiled(handed[:, :width], count)
    keep = keep_here * tiled(1.0 - handed[:, width:], count)
    both_o[rows:] = p
    mem = keep[:, :1] * tiled(mem_own[...], count) + mm(p.astype(BF16), wo[...])
    mem_o[...] = mem
    inverse = inverse_rms(mem)
    stat_o[0] = keep
    stat_o[1] = jnp.broadcast_to(inverse, (rows, LANES))
    mn = (mem * inverse * gain[...]).astype(BF16)
    both_o[:rows] = mn.astype(F32)
    kv_width = wk.shape[1]
    mkv_o[:, :kv_width] = mm(mn, wk[...]).astype(BF16).astype(F32)
    mkv_o[:, kv_width:] = mm(mn, wv[...]).astype(BF16).astype(F32)


def read_kernel(
    length, seg, cot, q, kv, mkv, wo, out_o, cr_o, dq_o, dkv_o, dmkv_o, dcr_s, cr_s
):
    count, width = q.shape
    slots = mkv.shape[0]
    kv_width = kv.shape[1] // 2
    pairs = width // LANES
    groups = kv_width // HEAD
    valid = lax.broadcasted_iota(jnp.int32, (count, 1), 0) < length[0, 0]
    d_out = jnp.where(valid, cot[...].astype(F32), 0.0).astype(BF16)
    dcr_s[...] = mm_nt(d_out, wo[...]).astype(BF16)
    key_at = lax.broadcasted_iota(jnp.int32, (slots + count, count), 0) - slots
    query_at = lax.broadcasted_iota(jnp.int32, (slots + count, count), 1)
    allowed = (key_at < 0) | ((key_at <= query_at) & (key_at < length[0, 0]))
    d_keys = [None] * groups
    d_values = [None] * groups
    for group in range(groups):
        at, odd = (group // 2) * LANES, group % 2
        keys = padded(
            jnp.concatenate(
                [mkv[:, at : at + LANES], kv[:, at : at + LANES].astype(F32)], axis=0
            ),
            odd,
        )
        at_v = kv_width + at
        values = padded(
            jnp.concatenate(
                [mkv[:, at_v : at_v + LANES], kv[:, at_v : at_v + LANES].astype(F32)], axis=0
            ),
            odd,
        )
        keys_t, values_t = keys.T, values.T
        dk = dv = None
        for pair in range(group * pairs // groups, (group + 1) * pairs // groups):
            lanes = slice(pair * LANES, (pair + 1) * LANES)
            q_tile = q[:, lanes]
            weights = softmax_rows(mm_nt(keys, q_tile), allowed)
            rounded = weights.astype(BF16)
            context = mm(values_t, rounded).T.astype(BF16)
            cr_s[:, lanes] = context
            cr_o[:, lanes] = context.astype(F32)
            d_tile = dcr_s[:, lanes]
            d_weights = mm_nt(values, d_tile).astype(BF16).astype(F32)
            d_scores = softmax_back(weights, d_weights).astype(BF16)
            dq = mm(keys_t, d_scores).T.astype(BF16).astype(F32)
            dq_o[:, lanes] = dq * score_scale
            dk_here = mm(d_scores, q_tile)
            dv_here = mm(rounded, d_tile)
            dk = dk_here if dk is None else dk + dk_here
            dv = dv_here if dv is None else dv + dv_here
        d_keys[group] = unpadded(dk, odd)
        d_values[group] = unpadded(dv, odd)
    for side, parts in ((0, d_keys), (kv_width, d_values)):
        for tile in range(groups // 2):
            lanes = slice(side + tile * LANES, side + (tile + 1) * LANES)
            total = (parts[2 * tile] + parts[2 * tile + 1]).astype(BF16).astype(F32)
            dmkv_o[:, lanes] = total[:slots]
            dkv_o[:, lanes] = total[slots:]
    out_o[...] = (seg[...].astype(F32) + mm(cr_s[...], wo[...])).astype(BF16)


def back_scan_kernel(
    place, dmkv, mem, ret, stat, mem_own, wo, wk, wv, gain,
    r_o, later_o, stat_o, end_o, g0_o, *, count,
):
    rows, width = mem.shape
    own = rows // count
    kv_width = wk.shape[1]
    dmb = dmkv[...].astype(BF16)
    dmn = mm_nt(dmb[:, :kv_width], wk[...]) + mm_nt(dmb[:, kv_width:], wv[...])
    inverse = stat[1][:, :1]
    keep = stat[0][:, :1]
    memory = mem[...]
    scaled = dmn * gain[...]
    inner = jnp.sum(scaled * memory, axis=1, keepdims=True) * (1.0 / width)
    r = inverse * scaled - memory * (inverse * inverse * inverse * inner)
    rounded = r.astype(BF16)
    r_o[...] = rounded.astype(F32)
    q = jnp.sum(r * tiled(mem_own[...], count), axis=1, keepdims=True)
    kept = keep * r
    g0 = kept[:own]
    for c in range(1, count):
        g0 = g0 + kept[c * own : (c + 1) * own]
    at = lax.broadcasted_iota(jnp.int32, (rows, 1), 0)
    first = place[0, 0] * own
    g0_o[...] = jnp.where((at >= first) & (at < first + own), tiled(g0, count), 0.0)
    turned = mm_nt(rounded, wo[...])
    q = jnp.broadcast_to(q, (rows, LANES))
    later = jnp.zeros((own, width), F32)
    later_q = jnp.zeros((own, LANES), F32)
    passed = jnp.ones((own, LANES), F32)
    for c in reversed(range(count)):
        at = slice(c * own, (c + 1) * own)
        retain = ret[0, at, :]
        later_o[at, :] = later
        stat_o[0, at, :] = later_q
        stat_o[1, at, :] = passed
        later = turned[at] + retain[:, :1] * later
        later_q = q[at] + retain * later_q
        passed = passed * retain
    end_o[:, :width] = later
    end_o[:, width:] = later_q


def back_kernel(later, stat_b, handed, both, call, ret, stat, u, wo, dc_o, vec_o, *, count):
    rows, width = later.shape
    passed = stat_b[1][:, :1]
    ahead = later[...] + passed * tiled(handed[:, :width], count)
    ahead_q = stat_b[0][:, :1] + passed * tiled(handed[:, width : width + 1], count)
    context = call[...]
    retain = ret[0][:, :1]
    d_retain = stat[0][:, :1] * ahead_q + jnp.sum(
        ahead * (both[rows:] - context), axis=1, keepdims=True
    )
    dz = d_retain * retain * (1.0 - retain)
    dc_o[...] = (1.0 - retain) * ahead + dz * u[...]
    v = jnp.sum(dz * context, axis=0, keepdims=True)
    vec_o[0:1, :] = v
    vec_o[1:2, :] = row_times(v, wo[...], False)


def finish_kernel(
    key, length, s, kv, dc, dkv_r, vec,
    dkv_o, keep_o, send_o, dqs_s,
):
    count, width = kv.shape[0], s.shape[1]
    slots = s.shape[0]
    pieces, piece, _ = dqs_s.shape
    kv_width = kv.shape[1] // 2
    pairs = width // LANES
    groups = kv_width // HEAD
    allowed = lax.broadcasted_iota(jnp.int32, (count, slots), 0) < length[0, 0]
    d_keys = [None] * groups
    d_values = [None] * groups
    for group in range(groups):
        at, odd = (group // 2) * LANES, group % 2
        keys = padded(kv[:, at : at + LANES], odd)
        values = padded(kv[:, kv_width + at : kv_width + at + LANES], odd)
        keys_t = keys.T
        dk = dv = None
        for pair in range(group * pairs // groups, (group + 1) * pairs // groups):
            lanes = slice(pair * LANES, (pair + 1) * LANES)
            s_tile = s[:, lanes]
            weights = softmax_rows(mm_nt(keys, s_tile), allowed)
            d_tile = dc[:, lanes].astype(BF16)
            d_weights = mm_nt(values, d_tile).astype(BF16).astype(F32)
            d_scores = softmax_back(weights, d_weights).astype(BF16)
            dqs = mm(keys_t, d_scores).T.astype(BF16).astype(F32)
            dqs = dqs * score_scale
            for t in range(pieces):
                dqs_s[t, :, lanes] = dqs[t * piece : (t + 1) * piece]
            dk_here = mm(d_scores, s_tile)
            dv_here = mm(weights.astype(BF16), d_tile)
            dk = dk_here if dk is None else dk + dk_here
            dv = dv_here if dv is None else dv + dv_here
        d_keys[group] = unpadded(dk, odd)
        d_values[group] = unpadded(dv, odd)
    for side, parts in ((0, d_keys), (kv_width, d_values)):
        for tile in range(groups // 2):
            lanes = slice(side + tile * LANES, side + (tile + 1) * LANES)
            total = (parts[2 * tile] + parts[2 * tile + 1]).astype(BF16).astype(F32)
            total = (total + dkv_r[:, lanes]).astype(BF16)
            dkv_o[:, lanes] = total.astype(F32)
    step = piece + 8
    sums = jnp.concatenate(
        [vec[...], jnp.zeros((6, width), F32)], axis=0
    )
    for t in range(pieces // 2):
        at = slice(t * step, t * step + piece)
        keep_o[at, :] = dqs_s[key[0, 0] ^ t]
        send_o[at, :] = dqs_s[key[0, 0] ^ (t + pieces // 2)]
        keep_o[t * step + piece : (t + 1) * step] = sums
        send_o[t * step + piece : (t + 1) * step] = sums


def last_kernel(
    key, me, near, far, sn, wq, mem0, gain, vector, kept, got, kept_out, got_out, kept_kv, got_kv,
    wq_rows, wk_rows, wv_rows,
    query_o, out_o, key_o, value_o, gain_o, gate_o, mem_o, dqs_s, turn_s,
):
    slots, width = sn.shape
    pieces, piece, _ = dqs_s.shape
    height = kept.shape[0]
    for t in range(pieces // 2):
        at = slice(t * (piece + 8), t * (piece + 8) + piece)
        dqs_s[key[0, 0] ^ t] = near[at]
        dqs_s[key[0, 0] ^ (t + pieces // 2)] = far[at]
    d_slots = jnp.concatenate([dqs_s[t] for t in range(pieces)], axis=0).astype(BF16)
    turned = sn[...].astype(F32).T
    for b in range(width // height):
        turn_s[b, :, :slots] = turned[b * height : (b + 1) * height]
    rows = turn_s[me[0, 0], :, :slots].astype(BF16)
    d_query = kept[...] + got[...] + mm(rows, d_slots)
    query_o[...] = d_query
    kv_width = key_o.shape[1]
    d_kv = kept_kv[...] + got_kv[...]
    key_o[...] = d_kv[:, :kv_width]
    value_o[...] = d_kv[:, kv_width:]
    scaled_gain = (
        jnp.sum(d_query * wq_rows[...].astype(F32), axis=1, keepdims=True)
        + jnp.sum(d_kv[:, :kv_width] * wk_rows[...].astype(F32), axis=1, keepdims=True)
        + jnp.sum(d_kv[:, kv_width:] * wv_rows[...].astype(F32), axis=1, keepdims=True)
    )
    dsn = mm_nt(d_slots, wq[...])
    start = mem0[...].astype(F32)
    inverse = inverse_rms(start)
    scaled = dsn * gain[...]
    inner = jnp.sum(scaled * start, axis=1, keepdims=True) * (1.0 / width)
    d_start = inverse * scaled - start * (inverse * inverse * inverse * inner)
    sums = near[piece : piece + 8]
    small = jnp.concatenate(
        [sums, gain[...], jnp.zeros((slots - 9, width), F32)], axis=0
    )
    columns = jnp.concatenate([d_start, small], axis=0).T
    for b in range(width // height):
        turn_s[b] = columns[b * height : (b + 1) * height]
    mine = turn_s[me[0, 0]]
    held = kept_out[:, width:] + got_out[:, width:]
    mem_o[...] = mine[:, :slots] + held
    lane = lax.broadcasted_iota(jnp.int32, (height, slots), 1)
    across = jnp.where(lane == 0, scaled_gain / mine[:, slots + 8 : slots + 9], mine[:, slots:]).T
    gain_o[...] = across[0:1]
    gate_o[...] = across[1:2]
    out_o[...] = (
        kept_out[:, :width]
        + got_out[:, :width]
        + mine[:, slots : slots + 1] * vector[...]
    )


def line_kernel(me, *refs, table, ranges):
    ins, out, turned = refs[:-2], refs[-2], refs[-1]
    blocks, height, _ = turned.shape
    lane = 0
    for i, first, last in ranges:
        across = slice(lane, lane + last - first)
        tall = ins[i][first:last].T
        for b in range(blocks):
            turned[b, :, across] = tall[b * height : (b + 1) * height]
        lane += last - first
    for b in range(blocks // 2):
        out[b * height : (b + 1) * height, :] = turned[me[0, 0] ^ table[b]].astype(BF16)


def product_kernel(me, *refs, plan):
    ins = refs[: plan["ins"]]
    outs = list(refs[plan["ins"] : -2])
    turned, lined = refs[-2:]
    blocks, height, _ = turned.shape
    kind = turned.dtype
    places, lane = {}, 0
    for _, _, items in plan["groups"]:
        for lefts, _, _ in items:
            for left in lefts:
                if left in places:
                    continue
                if left[0] == "line":
                    places[left] = (ins[left[1]], slice(left[2], left[3]))
                    continue
                i, first, last = left
                rows = ins[i][first:last].astype(kind)
                across = slice(lane, lane + last - first)
                places[left] = (lined, across)
                tall = rows.T
                for b in range(blocks):
                    turned[b, :, across] = tall[b * height : (b + 1) * height]
                lane += last - first
    base = plan["groups"][0][0]
    for b in range(blocks // 2 if lane else 0):
        lined[b * height : (b + 1) * height, :lane] = turned[me[0, 0] ^ base[b], :, :lane]
    where = {dest: b for b, dest in enumerate(base)}
    for table, pieces, items in plan["groups"]:
        size = blocks // 2 // pieces
        runs = []
        for dest in table:
            b = where[dest]
            if runs and runs[-1][1] == b:
                runs[-1][1] = b + 1
            else:
                runs.append([b, b + 1])
        offset = 0
        cuts = []
        for lo, hi in runs:
            while lo < hi:
                take = min(hi - lo, size - offset % size)
                cuts.append((offset, lo, lo + take))
                offset += take
                lo += take
        at = 0
        for lefts, rights, columns in items:
            if rights:
                right = jnp.concatenate(
                    [
                        ins[i][first:last, columns[0] : columns[1]].astype(BF16)
                        for i, first, last in rights
                    ],
                    axis=0,
                )
            for offset, lo, hi in cuts:
                out = outs[offset // size]
                first = offset % size * height
                to = slice(first, first + (hi - lo) * height)
                left = [
                    places[part][0][lo * height : hi * height, places[part][1]] for part in lefts
                ]
                if rights:
                    left = jnp.concatenate([part.astype(BF16) for part in left], axis=1)
                    out[to, at : at + right.shape[1]] = mm(left, right)
                else:
                    out[to, at : at + left[0].shape[1]] = sum(left[1:], left[0])
            at += columns[1] - columns[0]
        outs = outs[pieces:]


SMEM = pl.BlockSpec(memory_space=pltpu.SMEM)
VMEM = pl.BlockSpec(memory_space=pltpu.VMEM)


def call(kernel, scalars, arrays, outs, scratch=()):
    return pl.pallas_call(
        kernel,
        out_shape=tuple(jax.ShapeDtypeStruct(shape, kind) for shape, kind in outs),
        in_specs=[SMEM] * len(scalars) + [VMEM] * len(arrays),
        out_specs=tuple([VMEM] * len(outs)),
        scratch_shapes=[pltpu.VMEM(shape, kind) for shape, kind in scratch],
    )(*scalars, *arrays)


def per_device(
    chain,
    docs,
    segments,
    lengths,
    query_weight,
    key_weight,
    value_weight,
    out_weight,
    norm_gain,
    gate_vector,
    gate_bias,
    memory_init,
    cotangent,
):
    segment, cot = segments[0, 0], cotangent[0, 0]
    count, width = segment.shape
    slots = memory_init.shape[0]
    kv2 = 2 * key_weight.shape[1]
    count_half = chain // 2
    own = slots // count_half
    devices = chain * docs
    place = lax.axis_index("chain")
    me = (place * docs + lax.axis_index("dp")).reshape(1, 1)
    mine = place % count_half
    gain, vector = norm_gain[None, :], gate_vector[None, :]
    bias = lax.dynamic_slice(gate_bias, (mine * own,), (own,))[:, None]
    mem_own = lax.dynamic_slice(memory_init, (mine * own, 0), (own, width)).astype(F32)

    bits = devices.bit_length() - 1
    low = docs.bit_length() - 1
    others = list(range(low + 1, bits))
    within = list(range(low))
    order_a = within + others
    order_b = others[:1] + within + others[1:]
    meet = low + 1
    cut = width // 2
    height = width // devices

    def table_of(order):
        table = []
        for b in range(devices // 2):
            table.append(sum(((b >> (bits - 2 - k)) & 1) << pos for k, pos in enumerate(order)))
        return tuple(table)

    def products(arrays, groups):
        outs, plan, ranges = [], [], {}
        for order, pieces, items in groups:
            lanes = sum(columns[1] - columns[0] for _, _, columns in items)
            outs += [((width // 2 // pieces, lanes), F32)] * pieces
            for lefts, _, _ in items:
                ranges.update({left: left[2] - left[1] for left in lefts if left[0] != "line"})
            plan.append((table_of(order), pieces, items))
        tall = max(LANES, sum(ranges.values()))
        return call(
            functools.partial(product_kernel, plan={"ins": len(arrays), "groups": plan}),
            [me],
            arrays,
            outs,
            [((devices, height, tall), F32), ((width // 2, tall), F32)],
        )

    def line(arrays, ranges):
        tall = sum(last - first for _, first, last in ranges)
        return call(
            functools.partial(line_kernel, table=table_of(order_a), ranges=ranges),
            [me],
            arrays,
            [((width // 2, tall), BF16)],
            [((devices, height, tall), F32)],
        )[0]

    def swap(rows, pos):
        return lax.ppermute(rows, ("chain", "dp"), [(i, i ^ (1 << pos)) for i in range(devices)])

    spread = 1 << meet
    masks = [
        sum(((t >> (meet - 1 - k)) & 1) << pos for k, pos in enumerate(order_a[:meet]))
        for t in range(spread)
    ]

    def direct(sent):
        got = []
        for t, part in enumerate(sent):
            mask = masks[t + 1]
            got.append(
                lax.ppermute(
                    part, ("chain", "dp"), [(i, i ^ mask) for i in range(devices)]
                )
            )
        return got

    def split_sum(parts):
        half = parts[0].shape[0] // 2
        return sum(part[:half] for part in parts), sum(part[half:] for part in parts)

    def fold(kept, got):
        half = kept.shape[0] // 2
        return kept[:half] + got[:half], kept[half:] + got[half:]

    def halved(kept, sent, order):
        for pos in order[:-1]:
            kept, sent = fold(kept, swap(sent, pos))
        return kept, swap(sent, order[-1])

    def joined(pairs):
        halves = [fold(*pair) for pair in pairs]
        return tuple(jnp.concatenate([half[i] for half in halves], axis=1) for i in (0, 1))

    halves = [list(range(count_half)), list(range(count_half, chain))]

    def trade(blocks):
        return lax.all_to_all(
            blocks, "chain", 0, 0, axis_index_groups=halves, tiled=True
        )

    def handed(rows, back):
        pairs = [(c, c + count_half) for c in range(count_half)]
        return lax.ppermute(rows, "chain", [(b, a) if back else (a, b) for a, b in pairs])

    q, kv, sn, s, c = call(
        prepare_kernel,
        [lengths],
        [segment, query_weight, key_weight, value_weight, gain, memory_init],
        [
            ((count, width), BF16),
            ((count, kv2), BF16),
            ((slots, width), BF16),
            ((slots, width), BF16),
            ((slots, width), F32),
        ],
    )
    c_all = trade(c)
    pack0, u = call(
        rows_kernel,
        [lengths],
        [segment, cot, out_weight, gain, vector],
        [((2 * count, width), F32), ((1, width), F32)],
    )
    pack0_far = swap(pack0, low)
    p_here, ret, end = call(
        functools.partial(owner_scan_kernel, count=count_half),
        [],
        [c_all, bias, u],
        [
            ((slots, width), F32),
            ((2, slots, LANES), F32),
            ((own, width + LANES), F32),
        ],
    )
    entering = handed(end, False)
    pack1, mem, stat, mkv = call(
        functools.partial(owner_kernel, count=count_half),
        [],
        [p_here, ret, entering, mem_own, out_weight, key_weight, value_weight, gain],
        [
            ((2 * slots, width), F32),
            ((slots, width), F32),
            ((2, slots, LANES), F32),
            ((slots, kv2), F32),
        ],
    )
    mkv_here = trade(mkv)
    pack1_far = swap(pack1, low)
    out, cr, dq, dkv_r, dmkv = call(
        read_kernel,
        [lengths],
        [segment, cot, q, kv, mkv_here, out_weight],
        [
            ((count, width), BF16),
            ((count, width), F32),
            ((count, width), F32),
            ((count, kv2), F32),
            ((slots, kv2), F32),
        ],
        [((count, width), BF16), ((count, width), BF16)],
    )
    dq_far = swap(dq, low)
    cr_far = swap(cr, low)
    dmkv_all = trade(dmkv)

    def rows_of(i, first, size):
        return (i, first, first + size)

    lined0 = line([pack0, pack0_far], [rows_of(0, 0, count), rows_of(1, 0, count)])
    lined1 = line(
        [pack1, pack1_far],
        [
            rows_of(0, 0, slots), rows_of(1, 0, slots),
            rows_of(0, slots, slots), rows_of(1, slots, slots),
        ],
    )
    early_items = (
        (("line", 0, 0, 2 * count),),
        (rows_of(1, 0, count), rows_of(2, 0, count)),
    )

    def split(items, *more):
        lefts, rights = items
        return [
            (order_a, 2, [(lefts, rights, (0, cut))]),
            (order_b, 2, [(lefts, rights, (cut, width)), *more]),
        ]

    early, *sent = products([lined0, dq, dq_far], [(order_a, spread, [(*early_items, (0, width))])])
    early_far = direct(sent)
    early = split_sum([early, *early_far])
    r, later, stat_b, end, g0 = call(
        functools.partial(back_scan_kernel, count=count_half),
        [mine.reshape(1, 1)],
        [dmkv_all, mem, ret, stat, mem_own, out_weight, key_weight, value_weight, gain],
        [
            ((slots, width), F32),
            ((slots, width), F32),
            ((2, slots, LANES), F32),
            ((own, width + LANES), F32),
            ((slots, width), F32),
        ],
    )
    r_far = swap(r, low)
    entering = handed(end, True)
    dmkv_far = swap(dmkv_all, low)
    g0_far = swap(g0, low)
    out_lefts = (
        rows_of(0, 0, count), rows_of(1, 0, count), ("line", 2, 2 * slots, 4 * slots),
    )
    out_rights = (
        rows_of(3, count, count), rows_of(4, count, count), rows_of(5, 0, slots), rows_of(6, 0, slots),
    )
    out_a, sent_a, out_b, sent_b = products(
        [cr, cr_far, lined1, pack0, pack0_far, r, r_far, g0, g0_far],
        split(
            (out_lefts, out_rights),
            ((rows_of(7, 0, slots), rows_of(8, 0, slots)), (), (0, slots)),
        ),
    )
    out_a = halved(out_a, sent_a, order_a[:meet])
    out_b = halved(out_b, sent_b, order_b[:meet])
    early_kept, early_got = halved(*early, order_a[meet:])
    out_kept, out_got = halved(*joined([out_a, out_b]), order_a[meet:])
    dc, vec = call(
        functools.partial(back_kernel, count=count_half),
        [],
        [later, stat_b, entering, pack1, c_all, ret, stat, u, out_weight],
        [((slots, width), F32), ((2, width), F32)],
    )
    dc_here = trade(dc)
    slot_bits = [low] + order_a[:meet]
    parts = 1 << len(slot_bits)
    flat = me[0, 0]
    key = sum(
        ((flat >> pos) & 1) << (len(slot_bits) - 1 - k) for k, pos in enumerate(slot_bits)
    ).reshape(1, 1)
    step = slots // parts + 8
    dkv, kept_s, sent_s = call(
        finish_kernel,
        [key, lengths],
        [s, kv, dc_here, dkv_r, vec],
        [((count, kv2), F32)] + [((spread * step, width), F32)] * 2,
        [((parts, slots // parts, width), F32)],
    )
    got_s = swap(sent_s, low)
    dkv_far = swap(dkv, low)
    kv_left = (("line", 0, 0, 2 * count), ("line", 1, 0, 2 * slots))
    kv_right = (
        rows_of(2, 0, count), rows_of(3, 0, count), rows_of(4, 0, slots), rows_of(5, 0, slots),
    )
    late, *sent = products(
        [lined0, lined1, dkv, dkv_far, dmkv_all, dmkv_far],
        [(order_a, spread, [(kv_left, kv_right, (0, kv2))])],
    )
    mine_s, *sent_s = [
        kept_s[t * step : (t + 1) * step] + got_s[t * step : (t + 1) * step]
        for t in range(spread)
    ]
    total = sum(direct(sent_s), mine_s)
    for pos in order_a[meet:]:
        total = total + swap(total, pos)
    near = jnp.concatenate([total, *direct([total] * (spread - 1))], axis=0)
    far = swap(near, low)
    late, got = halved(*split_sum([late, *direct(sent)]), order_a[meet:])
    first = me[0, 0] * height
    own_rows = [
        lax.dynamic_slice(weight, (first, 0), (height, weight.shape[1]))
        for weight in (query_weight, key_weight, value_weight)
    ]
    g_query, g_out, g_key, g_value, g_gain, g_gate, g_mem = call(
        last_kernel,
        [key, me],
        [
            near, far, sn, query_weight, memory_init, gain, vector,
            early_kept, early_got, out_kept, out_got, late, got, *own_rows,
        ],
        [((height, width), F32)] * 2
        + [((height, kv2 // 2), F32)] * 2
        + [((1, height), F32)] * 2 + [((height, slots), F32)],
        [((parts, slots // parts, width), F32), ((devices, height, 2 * slots), F32)],
    )
    return (
        out[None, None],
        g_query,
        g_key,
        g_value,
        g_out,
        g_gain[0],
        g_gate[0],
        g_mem.T,
    )


def solution(mesh):
    in_specs = (
        P("dp", "chain", None, None),
        P("dp", "chain"),
        P(),
        P(),
        P(),
        P(),
        P(),
        P(),
        P(),
        P(),
        P("dp", "chain", None, None),
    )
    out_specs = (
        P("dp", "chain", None, None),
        P(("chain", "dp"), None),
        P(("chain", "dp"), None),
        P(("chain", "dp"), None),
        P(("chain", "dp"), None),
        P(("chain", "dp")),
        P(("chain", "dp")),
        P(None, ("chain", "dp")),
    )

    def step(*args):
        return per_device(mesh.shape["chain"], mesh.shape["dp"], *args)

    return jax.shard_map(
        step, mesh=mesh, in_specs=in_specs, out_specs=out_specs, check_vma=False
    )
```
